256 devices in a mesh: dp: 64 (over x, z_lo, y, core), sub: 4 (over z_hi).
Axes of the slice: x: 4, y: 4, z: 8 (z_hi: 4, z_lo: 2; z = z_hi * 2 + z_lo), core: 2. Of those that a mesh axis runs over, the one named last changes fastest.
Arguments:
- queries: float32 [16384, 1024], P(('dp', 'sub')), may hold values from -8 to 8
- passages: float32 [16384, 1024], P(('dp', 'sub')), may hold values from -8 to 8
- positives: int32 [16384], P(('dp', 'sub')), may hold values from 0 to 16383, each once
Outputs:
- losses: float32 [16384], P(('dp', 'sub'))
- query_grads: float32 [16384, 1024], P(('dp', 'sub'))
- passage_grads: float32 [16384, 1024], P(('dp', 'sub'))
The draws below stay inside these ranges and needn't reach their ends.
All inputs are finite; a program needn't handle non-finite values.
Results may differ from the reference program's by a relative error of at most 0.00185.
The reference program's roundings to bfloat16 on the way count: a program that leaves them out, or rounds other values in their place, can miss the bound.
Values may be sent and summed in bfloat16 or wider, within the bound.
No kernel may reach another device: no remote copies, remote signals or barrier semaphores. Data moves between devices by JAX's collectives and lax.ppermute only.
A program may use at most 128 MiB of HBM per device.

```python
import math
import jax
import jax.numpy as jnp
from jax import lax

D = 1024
BATCH = 16384


def embedding_pair(key):
    base = jax.random.fold_in(key, 41)
    streams = jax.random.split(base, 2)
    spread = (0.115 / math.sqrt(D)) ** 0.5
    queries = spread * jax.random.normal(streams[0], (BATCH, D), jnp.float32)
    passages = spread * jax.random.normal(streams[1], (BATCH, D), jnp.float32)
    return (jnp.clip(queries, -8.0, 8.0), jnp.clip(passages, -8.0, 8.0))


def draw_queries(key, part):
    return embedding_pair(key)[0]


def draw_passages(key, part):
    return embedding_pair(key)[1]


def setup_inputs(seed: int = 0) -> dict:
    splits = jax.random.split(jax.random.key(seed), 4)
    queries = draw_queries(jax.random.fold_in(splits[3], 71), 0)
    passages = draw_passages(jax.random.fold_in(splits[3], 71), 0)
    positives = jax.random.permutation(splits[2], BATCH).astype(jnp.int32)
    return {"queries": queries, "passages": passages, "positives": positives}


logit_scale = 20.0


def widen(values):
    return lax.optimization_barrier(values.astype(jnp.bfloat16)).astype(jnp.float32)


def reference(queries, passages, positives):
    query_wide = widen(queries)
    passage_wide = widen(passages)
    height = math.gcd(BATCH, 512)
    column_ids = jnp.arange(BATCH, dtype=jnp.int32)
    query_blocks = query_wide.reshape(BATCH // height, height, D)
    target_blocks = positives.astype(jnp.int32).reshape(BATCH // height, height)

    def advance(running, inputs):
        block_queries, block_targets = inputs
        scores = jnp.dot(block_queries, passage_wide.T, preferred_element_type=jnp.float32) * logit_scale
        highest = jnp.max(scores, axis=1)
        log_norm = highest + jnp.log(jnp.sum(jnp.exp(scores - highest[:, None]), axis=1))
        onehot = (column_ids[None, :] == block_targets[:, None]).astype(jnp.float32)
        positive_score = jnp.sum(onehot * scores, axis=1)
        weights = widen((jnp.exp(scores - log_norm[:, None]) - onehot) * logit_scale)
        block_grads = jnp.dot(weights, passage_wide, preferred_element_type=jnp.float32)
        running = running + jnp.dot(weights.T, block_queries, preferred_element_type=jnp.float32)
        return running, (log_norm - positive_score, block_grads)

    passage_grads, (losses, query_grads) = lax.scan(
        advance, jnp.zeros((BATCH, D), jnp.float32), (query_blocks, target_blocks))
    return losses.reshape(BATCH), query_grads.reshape(BATCH, D), passage_grads
```

```python
import jax
import jax.numpy as jnp
import numpy as np
from jax import lax
from jax.experimental import pallas as pl
from jax.experimental.pallas import tpu as pltpu
from jax.sharding import Mesh
from jax.sharding import PartitionSpec as P

AXES = ("x", "zl", "y", "c", "zh")
SIZES = {"x": 4, "zl": 2, "y": 4, "c": 2, "zh": 4}
XY = ("x", "y")
ZC = ("c", "zh", "zl")

logit_scale = 20.0
ROWS = 64
BLOCK = 1024
TILE = 256
PIECE = 72
VMEM = pl.BlockSpec(memory_space=pltpu.VMEM)


def along_z(value, shift):
    pairs = []
    for i in range(8):
        zl, zh = divmod(i, 4)
        to = (zh * 2 + zl + shift) % 8
        pairs.append((i, (to % 2) * 4 + to // 2))
    return lax.ppermute(value, ("zl", "zh"), pairs)


def to_partner(value):
    return lax.ppermute(value, "c", [(0, 1), (1, 0)])


def gather_along_z(own):
    half = 40
    up2, down2 = along_z(own, 2), along_z(own, -2)
    up1, down1 = along_z(own, 1), along_z(own, -1)
    up3, down3 = along_z(up2, 1), along_z(down2, -1)
    far_a, far_b = along_z(up2[:half], 2), along_z(down2[half:], -2)
    return jnp.concatenate([own, down1, down2, down3, far_a, far_b, up3, up2, up1])


def rolled(row, z, sign):
    for bit in (1, 2, 4):
        turned = pltpu.roll(row, (sign * bit * ROWS) % 512, 1)
        row = jnp.where((z & bit) != 0, turned, row)
    return row


def place():
    z = lax.axis_index("zh") * 2 + lax.axis_index("zl")
    return z, lax.axis_index("c")


def to_absolute(row, z, c):
    mine, other = rolled(row[:, :512], z, 1), rolled(row[:, 512:], z, 1)
    first = jnp.where(c == 0, mine, other)
    second = jnp.where(c == 0, other, mine)
    return jnp.concatenate([first, second], axis=1)


def to_relative(row, z, c):
    first, second = row[:, :512], row[:, 512:]
    mine = jnp.where(c == 0, first, second)
    other = jnp.where(c == 0, second, first)
    return jnp.concatenate([rolled(mine, z, -1), rolled(other, z, -1)], axis=1)


def scores_kernel(own_ref, other_ref, p_ref, q_ref, s_ref, target_ref, stats_ref):
    z, c = place()
    lane_block = lax.broadcasted_iota(jnp.int32, (1, BLOCK), 1) // ROWS
    high = jnp.zeros((1, BLOCK), jnp.float32)
    low = jnp.zeros((1, BLOCK), jnp.float32)
    for slot in range(16):
        ref, at = (own_ref, slot * PIECE) if slot < 8 else (other_ref, (slot - 8) * PIECE)
        q_ref[slot * ROWS : (slot + 1) * ROWS, :] = ref[at : at + ROWS, :]
        meta = ref[at + ROWS : at + PIECE, :].astype(jnp.float32)
        high = jnp.where(lane_block == slot, meta[0:1], high)
        low = jnp.where(lane_block == slot, meta[1:2], low)
    target = high.astype(jnp.int32) * 128 + low.astype(jnp.int32)
    here = (
        (((target >> 6) & 3) == lax.axis_index("zh"))
        & (((target >> 8) & 1) == c)
        & (((target >> 11) & 1) == lax.axis_index("zl"))
    )
    column = ((target >> 12) & 3) * 256 + ((target >> 9) & 3) * 64 + (target & 63)
    column = jnp.where(here, column, -1)
    target_ref[...] = column

    lse, positive = [], []
    for i in range(4):
        across = slice(i * TILE, (i + 1) * TILE)
        q_tile = q_ref[across, :]

        def score(j, carry):
            highest, pos = carry
            down = pl.ds(pl.multiple_of(j * TILE, TILE), TILE)
            s = logit_scale * lax.dot_general(
                p_ref[down, :], q_tile, (((1,), (1,)), ((), ())), preferred_element_type=jnp.float32
            )
            s_ref[down, across] = s
            row = lax.broadcasted_iota(jnp.int32, (TILE, TILE), 0) + j * TILE
            pos = pos + jnp.sum(jnp.where(row == column[:, across], s, 0.0), axis=0, keepdims=True)
            return jnp.maximum(highest, jnp.max(s, axis=0, keepdims=True)), pos

        start = (jnp.full((1, TILE), -jnp.inf, jnp.float32), jnp.zeros((1, TILE), jnp.float32))
        highest, pos = lax.fori_loop(0, 4, score, start)

        def total(j, acc):
            down = pl.ds(pl.multiple_of(j * TILE, TILE), TILE)
            return acc + jnp.sum(jnp.exp(s_ref[down, across] - highest), axis=0, keepdims=True)

        acc = lax.fori_loop(0, 4, total, jnp.zeros((1, TILE), jnp.float32))
        lse.append(highest + jnp.log(acc))
        positive.append(pos)
    for at, parts in ((0, lse), (8, positive)):
        row = to_absolute(jnp.concatenate(parts, axis=1), z, c)
        for r in range(8):
            stats_ref[at + r : at + r + 1, :] = row[:, r * 128 : (r + 1) * 128]


def weights_kernel(stats_ref, target_ref, s_ref, p_ref, w_ref, mine_ref, other_ref, loss_ref):
    z, c = place()
    stats = stats_ref[...]
    lses = stats[:, 0:8, :]
    highest = jnp.max(lses, axis=0)
    log_norm = highest + jnp.log(jnp.sum(jnp.exp(lses - highest[None]), axis=0))
    positive = jnp.sum(stats[:, 8:16, :], axis=0)
    flat = [
        to_relative(jnp.concatenate([v[r : r + 1] for r in range(8)], axis=1), z, c)
        for v in (log_norm, positive)
    ]
    log_norm = flat[0]
    loss_ref[...] = (flat[0] - flat[1])[:, 0:128]
    column = target_ref[...]
    for i in range(4):
        across = slice(i * TILE, (i + 1) * TILE)

        def weigh(j, _):
            down = pl.ds(pl.multiple_of(j * TILE, TILE), TILE)
            row = lax.broadcasted_iota(jnp.int32, (TILE, TILE), 0) + j * TILE
            onehot = jnp.where(row == column[:, across], 1.0, 0.0)
            w = (jnp.exp(s_ref[down, across] - log_norm[:, across]) - onehot) * logit_scale
            w_ref[down, across] = w.astype(jnp.bfloat16)
            return 0

        lax.fori_loop(0, 4, weigh, 0)
        out = mine_ref if i < 2 else other_ref
        at = (i % 2) * TILE

        def product(j, _):
            cols = pl.ds(pl.multiple_of(j * TILE, TILE), TILE)
            out[at : at + TILE, cols] = lax.dot_general(
                w_ref[:, across], p_ref[:, cols], (((0,), (0,)), ((), ())),
                preferred_element_type=jnp.float32,
            )
            return 0

        lax.fori_loop(0, 4, product, 0)


def passage_kernel(w_ref, q_ref, out_ref):
    def product(j, _):
        down = pl.ds(pl.multiple_of(j * TILE, TILE), TILE)
        out_ref[down, :] = jnp.dot(
            w_ref[down, :], q_ref[...], preferred_element_type=jnp.float32
        ).astype(jnp.bfloat16)
        return 0

    lax.fori_loop(0, 4, product, 0)


def cost(flops):
    return pl.CostEstimate(flops=flops, bytes_accessed=8 << 20, transcendentals=BLOCK * BLOCK)


def struct(shape, dtype):
    return jax.ShapeDtypeStruct(shape, dtype)


def body(queries, passages, positives):
    query_half = queries.astype(jnp.bfloat16)
    passage_half = passages.astype(jnp.bfloat16)
    width = queries.shape[1]
    index = jnp.tile(positives, BLOCK // ROWS)
    meta = jnp.stack([index >> 7, index & 127] + [jnp.zeros_like(index)] * 6).astype(jnp.bfloat16)
    p_block = lax.all_to_all(
        jnp.broadcast_to(passage_half[None], (16, ROWS, width)), XY, 0, 0, tiled=True
    ).reshape(BLOCK, width)
    own = gather_along_z(jnp.concatenate([query_half, meta]))
    other = to_partner(own)

    params = pltpu.CompilerParams(vmem_limit_bytes=40 << 20)
    q_block, scores, column, stats = pl.pallas_call(
        scores_kernel,
        out_shape=(
            struct((BLOCK, width), jnp.bfloat16),
            struct((BLOCK, BLOCK), jnp.float32),
            struct((1, BLOCK), jnp.int32),
            struct((16, 128), jnp.float32),
        ),
        in_specs=[VMEM] * 3,
        out_specs=(VMEM,) * 4,
        compiler_params=params,
        cost_estimate=cost(2 * BLOCK**3),
        name="scores",
    )(own, other, p_block)
    stats = lax.all_to_all(jnp.broadcast_to(stats[None], (16, 16, 128)), ZC, 0, 0, tiled=True)
    weights, mine, others, losses = pl.pallas_call(
        weights_kernel,
        out_shape=(
            struct((BLOCK, BLOCK), jnp.bfloat16),
            struct((BLOCK // 2, width), jnp.float32),
            struct((BLOCK // 2, width), jnp.float32),
            struct((1, 128), jnp.float32),
        ),
        in_specs=[VMEM] * 4,
        out_specs=(VMEM,) * 4,
        compiler_params=params,
        cost_estimate=cost(2 * BLOCK**3),
        name="weights",
    )(stats, column, scores, p_block)
    arrived = to_partner(others)
    p_terms = pl.pallas_call(
        passage_kernel,
        out_shape=struct((BLOCK, width), jnp.bfloat16),
        in_specs=[VMEM] * 2,
        out_specs=VMEM,
        compiler_params=params,
        cost_estimate=cost(2 * BLOCK**3),
        name="passage",
    )(weights, q_block)
    p_terms = lax.all_to_all(p_terms.reshape(16, ROWS, width), XY, 0, 0, tiled=True)
    passage_grads = jnp.sum(p_terms.astype(jnp.float32), axis=0)
    terms = mine + arrived
    halves = terms.astype(jnp.bfloat16)
    query_grads = terms[:ROWS]
    for slot in (4, 3, 5, 2, 6, 1, 7):
        piece = along_z(halves[slot * ROWS : (slot + 1) * ROWS], slot)
        query_grads = query_grads + piece.astype(jnp.float32)
    return losses[0, :ROWS], query_grads, passage_grads


def solution(mesh):
    torus = Mesh(mesh.devices.reshape(4, 2, 4, 2, 4), AXES)
    placed = (P(AXES, None), P(AXES, None), P(AXES))
    return jax.shard_map(
        body,
        mesh=torus,
        in_specs=placed,
        out_specs=(P(AXES), P(AXES, None), P(AXES, None)),
        check_vma=False,
    )
```

```python
import functools

import jax
import jax.numpy as jnp
import numpy as np
from jax import lax
from jax.experimental import pallas as pl
from jax.experimental.pallas import tpu as pltpu
from jax.sharding import Mesh
from jax.sharding import PartitionSpec as P

AXES = ("x", "zl", "y", "c", "zh")
SIZES = {"x": 4, "zl": 2, "y": 4, "c": 2, "zh": 4}
XY = ("x", "y")
ZC = ("c", "zh", "zl")

logit_scale = 20.0
ROWS = 64
BLOCK = 1024
TILE = 256
PIECE = 72
VMEM = pl.BlockSpec(memory_space=pltpu.VMEM)


def along_z(value, shift):
    pairs = []
    for i in range(8):
        zl, zh = divmod(i, 4)
        to = (zh * 2 + zl + shift) % 8
        pairs.append((i, (to % 2) * 4 + to // 2))
    return lax.ppermute(value, ("zl", "zh"), pairs)


def to_partner(value):
    return lax.ppermute(value, "c", [(0, 1), (1, 0)])


def gather_along_z(own):
    half = 40
    up2, down2 = along_z(own, 2), along_z(own, -2)
    up1, down1 = along_z(own, 1), along_z(own, -1)
    up3, down3 = along_z(up2, 1), along_z(down2, -1)
    far_a, far_b = along_z(up2[:half], 2), along_z(down2[half:], -2)
    pieces = (own, down1, down2, down3, far_a, far_b, up3, up2, up1)
    return call(
        join_kernel, "join", pieces, struct((8 * PIECE, own.shape[1]), jnp.bfloat16), VMEM, limit=8
    )


def rolled(row, z, sign):
    for bit in (1, 2, 4):
        turned = pltpu.roll(row, (sign * bit * ROWS) % 512, 1)
        row = jnp.where((z & bit) != 0, turned, row)
    return row


def place():
    z = lax.axis_index("zh") * 2 + lax.axis_index("zl")
    return z, lax.axis_index("c")


def to_absolute(row, z, c):
    mine, other = rolled(row[:, :512], z, 1), rolled(row[:, 512:], z, 1)
    first = jnp.where(c == 0, mine, other)
    second = jnp.where(c == 0, other, mine)
    return jnp.concatenate([first, second], axis=1)


def to_relative(row, z, c):
    first, second = row[:, :512], row[:, 512:]
    mine = jnp.where(c == 0, first, second)
    other = jnp.where(c == 0, second, first)
    return jnp.concatenate([rolled(mine, z, -1), rolled(other, z, -1)], axis=1)


def prepare_kernel(q_in, p_in, positive_ref, q_ref, p_ref, half_ref, sems):
    half_ref[...] = p_in[...].astype(jnp.bfloat16)
    copies = [pltpu.make_async_copy(half_ref, p_ref.at[i], sems.at[i]) for i in range(16)]
    for copy in copies:
        copy.start()
    q_ref[:ROWS, :] = q_in[...].astype(jnp.bfloat16)
    index = positive_ref[...]
    index = jnp.concatenate([index] * 8, axis=1)
    row = lax.broadcasted_iota(jnp.int32, (PIECE - ROWS, BLOCK), 0)
    meta = jnp.where(row == 0, index >> 7, jnp.where(row == 1, index & 127, 0))
    q_ref[ROWS:, :] = meta.astype(jnp.float32).astype(jnp.bfloat16)
    for copy in copies:
        copy.wait()


def join_kernel(*refs):
    out_ref, at = refs[-1], 0
    for ref in refs[:-1]:
        rows = ref.shape[0]
        out_ref[at : at + rows, :] = ref[...]
        at += rows


def queries_kernel(own_ref, other_ref, q_ref, target_ref):
    lane_block = lax.broadcasted_iota(jnp.int32, (1, BLOCK), 1) // ROWS
    high = jnp.zeros((1, BLOCK), jnp.float32)
    low = jnp.zeros((1, BLOCK), jnp.float32)
    for slot in range(16):
        ref, at = (own_ref, slot * PIECE) if slot < 8 else (other_ref, (slot - 8) * PIECE)
        q_ref[slot * ROWS : (slot + 1) * ROWS, :] = ref[at : at + ROWS, :]
        meta = ref[at + ROWS : at + PIECE, :].astype(jnp.float32)
        high = jnp.where(lane_block == slot, meta[0:1], high)
        low = jnp.where(lane_block == slot, meta[1:2], low)
    target = high.astype(jnp.int32) * 128 + low.astype(jnp.int32)
    here = (
        (((target >> 6) & 3) == lax.axis_index("zh"))
        & (((target >> 8) & 1) == lax.axis_index("c"))
        & (((target >> 11) & 1) == lax.axis_index("zl"))
    )
    column = ((target >> 12) & 3) * 256 + ((target >> 9) & 3) * 64 + (target & 63)
    target_ref[...] = jnp.where(here, column, -1)


def tile(k):
    return slice(k * TILE, (k + 1) * TILE)


def scores_kernel(q_ref, target_ref, p_ref, s_ref, stats_ref):
    z, c = place()
    lse, positive = [], []
    for i in range(4):
        column = target_ref[:, tile(i)]
        highest = jnp.full((1, TILE), -jnp.inf, jnp.float32)
        pos = jnp.zeros((1, TILE), jnp.float32)
        for j in range(4):
            s = logit_scale * lax.dot_general(
                p_ref[tile(j), :], q_ref[tile(i), :], (((1,), (1,)), ((), ())),
                preferred_element_type=jnp.float32,
            )
            s_ref[tile(j), tile(i)] = s
            row = lax.broadcasted_iota(jnp.int32, (TILE, TILE), 0) + j * TILE
            pos = pos + jnp.sum(jnp.where(row == column, s, 0.0), axis=0, keepdims=True)
            highest = jnp.maximum(highest, jnp.max(s, axis=0, keepdims=True))
        acc = jnp.zeros((1, TILE), jnp.float32)
        for j in range(4):
            acc = acc + jnp.sum(jnp.exp(s_ref[tile(j), tile(i)] - highest), axis=0, keepdims=True)
        lse.append(highest + jnp.log(acc))
        positive.append(pos)
    for at, parts in ((0, lse), (8, positive)):
        row = to_absolute(jnp.concatenate(parts, axis=1), z, c)
        for r in range(8):
            stats_ref[at + r : at + r + 1, :] = row[:, r * 128 : (r + 1) * 128]


def weights_kernel(stats_ref, target_ref, s_ref, q_ref, w_ref, out_ref, loss_ref):
    z, c = place()
    stats = stats_ref[...]
    lses = stats[:, 0:8, :]
    highest = jnp.max(lses, axis=0)
    log_norm = highest + jnp.log(jnp.sum(jnp.exp(lses - highest[None]), axis=0))
    positive = jnp.sum(stats[:, 8:16, :], axis=0)
    log_norm, positive = (
        to_relative(jnp.concatenate([v[r : r + 1] for r in range(8)], axis=1), z, c)
        for v in (log_norm, positive)
    )
    loss_ref[...] = (log_norm - positive)[:, 0:128]
    for j in range(4):
        for i in range(4):
            row = lax.broadcasted_iota(jnp.int32, (TILE, TILE), 0) + j * TILE
            onehot = jnp.where(row == target_ref[:, tile(i)], 1.0, 0.0)
            w = (jnp.exp(s_ref[tile(j), tile(i)] - log_norm[:, tile(i)]) - onehot) * logit_scale
            w_ref[tile(j), tile(i)] = w.astype(jnp.bfloat16)
        for k in range(4):
            out_ref[tile(j), tile(k)] = jnp.dot(
                w_ref[tile(j), :], q_ref[:, tile(k)], preferred_element_type=jnp.float32
            ).astype(jnp.bfloat16)


def query_kernel(first, w_ref, p_ref, out_ref):
    for i in range(2):
        for k in range(4):
            out_ref[tile(i), tile(k)] = lax.dot_general(
                w_ref[:, tile(first + i)], p_ref[:, tile(k)], (((0,), (0,)), ((), ())),
                preferred_element_type=jnp.float32,
            )


def split_kernel(mine_ref, arrived_ref, own_ref, *outs):
    own_ref[...] = mine_ref[:ROWS, :] + arrived_ref[:ROWS, :]
    for slot in range(1, 8):
        at = slice(slot * ROWS, (slot + 1) * ROWS)
        outs[slot - 1][...] = (mine_ref[at, :] + arrived_ref[at, :]).astype(jnp.bfloat16)


def cost(flops, count):
    return pl.CostEstimate(flops=flops, bytes_accessed=count, transcendentals=0)


def struct(shape, dtype):
    return jax.ShapeDtypeStruct(shape, dtype)


def call(kernel, name, args, out_shape, out_specs, limit, flops=1 << 28, scratch=()):
    return pl.pallas_call(
        kernel,
        out_shape=out_shape,
        in_specs=[VMEM] * len(args),
        out_specs=out_specs,
        scratch_shapes=scratch,
        compiler_params=pltpu.CompilerParams(vmem_limit_bytes=limit << 20),
        cost_estimate=cost(flops, 4 << 20),
        name=name,
    )(*args)


def body(queries, passages, positives):
    width = queries.shape[1]
    matmul = 2 * BLOCK**3
    own, p_sent = call(
        prepare_kernel,
        "prepare",
        (queries, passages, jnp.tile(positives, 2).reshape(1, 128)),
        (struct((PIECE, width), jnp.bfloat16), struct((16, ROWS, width), jnp.bfloat16)),
        (VMEM, pl.BlockSpec(memory_space=pl.ANY)),
        limit=4,
        scratch=(pltpu.VMEM((ROWS, width), jnp.bfloat16), pltpu.SemaphoreType.DMA((16,))),
    )
    p_block = lax.all_to_all(p_sent, XY, 0, 0, tiled=True).reshape(BLOCK, width)
    gathered = gather_along_z(own)
    partner = to_partner(gathered)
    q_block, column = call(
        queries_kernel,
        "queries",
        (gathered, partner),
        (struct((BLOCK, width), jnp.bfloat16), struct((1, BLOCK), jnp.int32)),
        (VMEM, VMEM),
        limit=8,
    )
    scores, stats = call(
        scores_kernel,
        "scores",
        (q_block, column, p_block),
        (struct((BLOCK, BLOCK), jnp.float32), struct((16, 128), jnp.float32)),
        (VMEM, VMEM),
        limit=16,
        flops=matmul,
    )
    stats = lax.all_to_all(jnp.broadcast_to(stats[None], (16, 16, 128)), ZC, 0, 0, tiled=True)
    weights, p_terms, losses = call(
        weights_kernel,
        "weights",
        (stats, column, scores, q_block),
        (
            struct((BLOCK, BLOCK), jnp.bfloat16),
            struct((BLOCK, width), jnp.bfloat16),
            struct((1, 128), jnp.float32),
        ),
        (VMEM, VMEM, VMEM),
        limit=16,
        flops=matmul,
    )
    p_terms = lax.all_to_all(p_terms.reshape(16, ROWS, width), XY, 0, 0, tiled=True)
    half = struct((BLOCK // 2, width), jnp.float32)
    mine, others = (
        call(
            functools.partial(query_kernel, first),
            name,
            (weights, p_block),
            half,
            VMEM,
            limit=12,
            flops=matmul // 2,
        )
        for first, name in ((0, "mine"), (2, "others"))
    )
    own_terms, *pieces = call(
        split_kernel,
        "split",
        (mine, to_partner(others)),
        (struct((ROWS, width), jnp.float32),) + (struct((ROWS, width), jnp.bfloat16),) * 7,
        (VMEM,) * 8,
        limit=8,
    )
    arrived = {slot: along_z(pieces[slot - 1], slot) for slot in (4, 3, 5, 2, 6, 1, 7)}
    query_grads = own_terms
    for piece in arrived.values():
        query_grads = query_grads + piece.astype(jnp.float32)
    passage_grads = jnp.sum(p_terms.astype(jnp.float32), axis=0)
    return losses[0, :ROWS], query_grads, passage_grads


def solution(mesh):
    torus = Mesh(mesh.devices.reshape(4, 2, 4, 2, 4), AXES)
    placed = (P(AXES, None), P(AXES, None), P(AXES))
    return jax.shard_map(
        body,
        mesh=torus,
        in_specs=placed,
        out_specs=(P(AXES), P(AXES, None), P(AXES, None)),
        check_vma=False,
    )
```

```python
import functools

import jax
import jax.numpy as jnp
import numpy as np
from jax import lax
from jax.experimental import pallas as pl
from jax.experimental.pallas import tpu as pltpu
from jax.sharding import Mesh
from jax.sharding import PartitionSpec as P

AXES = ("x", "zl", "y", "c", "zh")
SIZES = {"x": 4, "zl": 2, "y": 4, "c": 2, "zh": 4}
XY = ("x", "y")
ZC = ("c", "zh", "zl")

logit_scale = 20.0
ROWS = 64
BLOCK = 1024
TILE = 256
PIECE = 72
VMEM = pl.BlockSpec(memory_space=pltpu.VMEM)
HBM = pl.BlockSpec(memory_space=pltpu.HBM)


def along_z(value, shift):
    pairs = []
    for i in range(8):
        zl, zh = divmod(i, 4)
        to = (zh * 2 + zl + shift) % 8
        pairs.append((i, (to % 2) * 4 + to // 2))
    return lax.ppermute(value, ("zl", "zh"), pairs)


def to_partner(value):
    return lax.ppermute(value, "c", [(0, 1), (1, 0)])


def gather_along_z(own):
    half = 40
    up2, down2 = along_z(own, 2), along_z(own, -2)
    up1, down1 = along_z(own, 1), along_z(own, -1)
    up3, down3 = along_z(up2, 1), along_z(down2, -1)
    far_a, far_b = along_z(up2[:half], 2), along_z(down2[half:], -2)
    pieces = (own, down1, down2, down3, far_a, far_b, up3, up2, up1)
    return call(
        join_kernel, "join", pieces, struct((8 * PIECE, own.shape[1]), jnp.bfloat16), VMEM, limit=8
    )


def rolled(row, z, sign):
    for bit in (1, 2, 4):
        turned = pltpu.roll(row, (sign * bit * ROWS) % 512, 1)
        row = jnp.where((z & bit) != 0, turned, row)
    return row


def place():
    z = lax.axis_index("zh") * 2 + lax.axis_index("zl")
    return z, lax.axis_index("c")


def to_absolute(row, z, c):
    mine, other = rolled(row[:, :512], z, 1), rolled(row[:, 512:], z, 1)
    first = jnp.where(c == 0, mine, other)
    second = jnp.where(c == 0, other, mine)
    return jnp.concatenate([first, second], axis=1)


def to_relative(row, z, c):
    first, second = row[:, :512], row[:, 512:]
    mine = jnp.where(c == 0, first, second)
    other = jnp.where(c == 0, second, first)
    return jnp.concatenate([rolled(mine, z, -1), rolled(other, z, -1)], axis=1)


def prepare_kernel(q_in, p_in, positive_in, q_ref, p_ref, q_wide, p_wide, half_ref, index_ref, sems):
    loads = [
        pltpu.make_async_copy(p_in, p_wide, sems.at[16]),
        pltpu.make_async_copy(q_in, q_wide, sems.at[17]),
        pltpu.make_async_copy(positive_in, index_ref, sems.at[18]),
    ]
    for load in loads:
        load.start()
    loads[0].wait()
    half_ref[...] = p_wide[...].astype(jnp.bfloat16)
    copies = [pltpu.make_async_copy(half_ref, p_ref.at[i], sems.at[i]) for i in range(16)]
    for copy in copies:
        copy.start()
    loads[1].wait()
    q_ref[:ROWS, :] = q_wide[...].astype(jnp.bfloat16)
    loads[2].wait()
    index = index_ref[...]
    index = jnp.concatenate([index] * 16, axis=1)
    row = lax.broadcasted_iota(jnp.int32, (PIECE - ROWS, BLOCK), 0)
    meta = jnp.where(row == 0, index >> 7, jnp.where(row == 1, index & 127, 0))
    q_ref[ROWS:, :] = meta.astype(jnp.float32).astype(jnp.bfloat16)
    for copy in copies:
        copy.wait()


def join_kernel(*refs):
    out_ref, at = refs[-1], 0
    for ref in refs[:-1]:
        rows = ref.shape[0]
        out_ref[at : at + rows, :] = ref[...]
        at += rows


def tile(k):
    return slice(k * TILE, (k + 1) * TILE)


def scores_kernel(own_ref, other_ref, p_in, q_ref, p_ref, target_ref, s_ref, stats_ref, sems):
    loads = [pltpu.make_async_copy(p_in.at[tile(j)], p_ref.at[tile(j)], sems.at[j]) for j in range(4)]
    for load in loads:
        load.start()
    z, c = place()
    lane_block = lax.broadcasted_iota(jnp.int32, (1, BLOCK), 1) // ROWS
    high = jnp.zeros((1, BLOCK), jnp.float32)
    low = jnp.zeros((1, BLOCK), jnp.float32)
    for slot in range(16):
        ref, at = (own_ref, slot * PIECE) if slot < 8 else (other_ref, (slot - 8) * PIECE)
        q_ref[slot * ROWS : (slot + 1) * ROWS, :] = ref[at : at + ROWS, :]
        meta = ref[at + ROWS : at + PIECE, :].astype(jnp.float32)
        high = jnp.where(lane_block == slot, meta[0:1], high)
        low = jnp.where(lane_block == slot, meta[1:2], low)
    target = high.astype(jnp.int32) * 128 + low.astype(jnp.int32)
    here = (
        (((target >> 6) & 3) == lax.axis_index("zh"))
        & (((target >> 8) & 1) == c)
        & (((target >> 11) & 1) == lax.axis_index("zl"))
    )
    column = ((target >> 12) & 3) * 256 + ((target >> 9) & 3) * 64 + (target & 63)
    target_ref[...] = jnp.where(here, column, -1)

    lse, positive = [], []
    for i in range(4):
        column = target_ref[:, tile(i)]
        highest = jnp.full((1, TILE), -jnp.inf, jnp.float32)
        pos = jnp.zeros((1, TILE), jnp.float32)
        for j in range(4):
            if i == 0:
                loads[j].wait()
            s = logit_scale * lax.dot_general(
                p_ref[tile(j), :], q_ref[tile(i), :], (((1,), (1,)), ((), ())),
                preferred_element_type=jnp.float32,
            )
            s_ref[tile(j), tile(i)] = s
            row = lax.broadcasted_iota(jnp.int32, (TILE, TILE), 0) + j * TILE
            pos = pos + jnp.sum(jnp.where(row == column, s, 0.0), axis=0, keepdims=True)
            highest = jnp.maximum(highest, jnp.max(s, axis=0, keepdims=True))
        acc = jnp.zeros((1, TILE), jnp.float32)
        for j in range(4):
            acc = acc + jnp.sum(jnp.exp(s_ref[tile(j), tile(i)] - highest), axis=0, keepdims=True)
        lse.append(highest + jnp.log(acc))
        positive.append(pos)
    for at, parts in ((0, lse), (8, positive)):
        row = to_absolute(jnp.concatenate(parts, axis=1), z, c)
        for r in range(8):
            stats_ref[0, at + r : at + r + 1, :] = row[:, r * 128 : (r + 1) * 128]
    for k in range(1, 16):
        stats_ref[k] = stats_ref[0]


def weights_kernel(
    stats_ref, target_ref, s_ref, q_ref, p_ref, out_ref, mine_ref, other_ref, loss_ref,
    w_ref, terms_ref, sums_ref, sems,
):
    z, c = place()
    stats = stats_ref[...]
    lses = stats[:, 0:8, :]
    highest = jnp.max(lses, axis=0)
    log_norm = highest + jnp.log(jnp.sum(jnp.exp(lses - highest[None]), axis=0))
    positive = jnp.sum(stats[:, 8:16, :], axis=0)
    log_norm, positive = (
        to_relative(jnp.concatenate([v[r : r + 1] for r in range(8)], axis=1), z, c)
        for v in (log_norm, positive)
    )
    loss_ref[...] = (log_norm - positive)[:, 0:ROWS]
    stores = []
    for j in range(4):
        for i in range(4):
            row = lax.broadcasted_iota(jnp.int32, (TILE, TILE), 0) + j * TILE
            onehot = jnp.where(row == target_ref[:, tile(i)], 1.0, 0.0)
            w = (jnp.exp(s_ref[tile(j), tile(i)] - log_norm[:, tile(i)]) - onehot) * logit_scale
            w_ref[tile(j), tile(i)] = w.astype(jnp.bfloat16)
        for k in range(4):
            terms_ref[tile(j), tile(k)] = jnp.dot(
                w_ref[tile(j), :], q_ref[:, tile(k)], preferred_element_type=jnp.float32
            ).astype(jnp.bfloat16)
        stores.append(pltpu.make_async_copy(terms_ref.at[tile(j)], out_ref.at[tile(j)], sems.at[j]))
        stores[-1].start()
    for i in (2, 3, 0, 1):
        for k in range(4):
            product = lax.dot_general(
                w_ref[:, tile(i)], p_ref[:, tile(k)], (((0,), (0,)), ((), ())),
                preferred_element_type=jnp.float32,
            )
            if i >= 2:
                other_ref[tile(i - 2), tile(k)] = product
            else:
                sums_ref[tile(i), tile(k)] = product
        if i < 2:
            stores.append(
                pltpu.make_async_copy(sums_ref.at[tile(i)], mine_ref.at[tile(i)], sems.at[4 + i])
            )
            stores[-1].start()
    for store in stores:
        store.wait()


def split_kernel(mine_in, arrived_ref, own_ref, *rest):
    outs, mine_ref, sems = rest[:7], rest[7], rest[8]
    rows = [slice(slot * ROWS, (slot + 1) * ROWS) for slot in range(8)]
    loads = [pltpu.make_async_copy(mine_in.at[r], mine_ref.at[r], sems.at[i]) for i, r in enumerate(rows)]
    for load in loads:
        load.start()
    for slot, at in enumerate(rows):
        loads[slot].wait()
        total = mine_ref[at, :] + arrived_ref[at, :]
        if slot == 0:
            own_ref[...] = total
        else:
            outs[slot - 1][...] = total.astype(jnp.bfloat16)


def total_kernel(p_in, own_ref, *rest):
    pieces, (q_out, p_out), (p_ref, sum_ref, sems) = rest[:7], rest[7:9], rest[9:]
    loads = [pltpu.make_async_copy(p_in.at[i], p_ref.at[i], sems.at[i]) for i in range(16)]
    for load in loads:
        load.start()
    total = own_ref[...]
    for piece in pieces:
        total = total + piece[...].astype(jnp.float32)
    sum_ref[0] = total
    store = pltpu.make_async_copy(sum_ref.at[0], q_out, sems.at[16])
    store.start()
    for load in loads:
        load.wait()
    total = p_ref[0].astype(jnp.float32)
    for i in range(1, 16):
        total = total + p_ref[i].astype(jnp.float32)
    sum_ref[1] = total
    last = pltpu.make_async_copy(sum_ref.at[1], p_out, sems.at[17])
    last.start()
    store.wait()
    last.wait()


def cost(flops, count):
    return pl.CostEstimate(flops=flops, bytes_accessed=count, transcendentals=0)


def struct(shape, dtype):
    return jax.ShapeDtypeStruct(shape, dtype)


def far(shape, dtype):
    return pltpu.HBM(shape, dtype)


def call(kernel, name, args, out_shape, out_specs, limit, flops=1 << 28, scratch=(), held=()):
    return pl.pallas_call(
        kernel,
        out_shape=out_shape,
        in_specs=[HBM if i in held else VMEM for i in range(len(args))],
        out_specs=out_specs,
        scratch_shapes=scratch,
        compiler_params=pltpu.CompilerParams(vmem_limit_bytes=limit << 20),
        cost_estimate=cost(flops, 4 << 20),
        name=name,
    )(*(pltpu.with_memory_space_constraint(a, pltpu.HBM) if i in held else a for i, a in enumerate(args)))


def body(queries, passages, positives):
    width = queries.shape[1]
    matmul = 2 * BLOCK**3
    own, p_sent = call(
        prepare_kernel,
        "prepare",
        (queries, passages, positives.reshape(1, ROWS)),
        (struct((PIECE, width), jnp.bfloat16), far((16, ROWS, width), jnp.bfloat16)),
        (VMEM, HBM),
        limit=4,
        scratch=(
            pltpu.VMEM((ROWS, width), jnp.float32),
            pltpu.VMEM((ROWS, width), jnp.float32),
            pltpu.VMEM((ROWS, width), jnp.bfloat16),
            pltpu.VMEM((1, ROWS), jnp.int32),
            pltpu.SemaphoreType.DMA((19,)),
        ),
        held=(0, 1, 2),
    )
    p_block = lax.all_to_all(p_sent, XY, 0, 0, tiled=True).reshape(BLOCK, width)
    gathered = gather_along_z(own)
    partner = to_partner(gathered)
    q_block, p_block, column, scores, stats = call(
        scores_kernel,
        "scores",
        (gathered, partner, p_block),
        (
            struct((BLOCK, width), jnp.bfloat16),
            struct((BLOCK, width), jnp.bfloat16),
            struct((1, BLOCK), jnp.int32),
            struct((BLOCK, BLOCK), jnp.float32),
            struct((16, 16, 128), jnp.float32),
        ),
        (VMEM,) * 5,
        limit=20,
        flops=matmul,
        scratch=(pltpu.SemaphoreType.DMA((4,)),),
        held=(2,),
    )
    stats = lax.all_to_all(stats, ZC, 0, 0, tiled=True)
    half = (BLOCK // 2, width)
    p_terms, mine, others, losses = call(
        weights_kernel,
        "weights",
        (stats, column, scores, q_block, p_block),
        (
            far((BLOCK, width), jnp.bfloat16),
            far(half, jnp.float32),
            struct(half, jnp.float32),
            struct((1, ROWS), jnp.float32),
        ),
        (HBM, HBM, VMEM, VMEM),
        limit=30,
        flops=2 * matmul,
        scratch=(
            pltpu.VMEM((BLOCK, BLOCK), jnp.bfloat16),
            pltpu.VMEM((BLOCK, width), jnp.bfloat16),
            pltpu.VMEM(half, jnp.float32),
            pltpu.SemaphoreType.DMA((6,)),
        ),
    )
    p_terms = lax.all_to_all(p_terms.reshape(16, ROWS, width), XY, 0, 0, tiled=True)
    block = (ROWS, width)
    own_terms, *pieces = call(
        split_kernel,
        "split",
        (mine, to_partner(others)),
        (struct(block, jnp.float32),) + (struct(block, jnp.bfloat16),) * 7,
        (VMEM,) * 8,
        limit=8,
        scratch=(pltpu.VMEM(half, jnp.float32), pltpu.SemaphoreType.DMA((8,))),
        held=(0,),
    )
    arrived = [along_z(piece, slot) for slot, piece in enumerate(pieces, 1)]
    query_grads, passage_grads = call(
        total_kernel,
        "total",
        (p_terms, own_terms, *arrived),
        (far(block, jnp.float32),) * 2,
        (HBM,) * 2,
        limit=8,
        scratch=(
            pltpu.VMEM((16, *block), jnp.bfloat16),
            pltpu.VMEM((2, *block), jnp.float32),
            pltpu.SemaphoreType.DMA((18,)),
        ),
        held=(0,),
    )
    return losses.reshape(ROWS), query_grads, passage_grads


def solution(mesh):
    torus = Mesh(mesh.devices.reshape(4, 2, 4, 2, 4), AXES)
    placed = (P(AXES, None), P(AXES, None), P(AXES))
    return jax.shard_map(
        body,
        mesh=torus,
        in_specs=placed,
        out_specs=(P(AXES), P(AXES, None), P(AXES, None)),
        check_vma=False,
    )
```

```python
import functools

import jax
import jax.numpy as jnp
import numpy as np
from jax import lax
from jax.experimental import pallas as pl
from jax.experimental.pallas import tpu as pltpu
from jax.sharding import Mesh
from jax.sharding import PartitionSpec as P

AXES = ("x", "zl", "y", "c", "zh")
SIZES = {"x": 4, "zl": 2, "y": 4, "c": 2, "zh": 4}
XY = ("x", "y")
ZC = ("c", "zh", "zl")

logit_scale = 20.0
ROWS = 64
BLOCK = 1024
TILE = 256
PIECE = 72
VMEM = pl.BlockSpec(memory_space=pltpu.VMEM)
HBM = pl.BlockSpec(memory_space=pltpu.HBM)


def along_z(value, shift):
    pairs = []
    for i in range(8):
        zl, zh = divmod(i, 4)
        to = (zh * 2 + zl + shift) % 8
        pairs.append((i, (to % 2) * 4 + to // 2))
    return lax.ppermute(value, ("zl", "zh"), pairs)


def to_partner(value):
    return lax.ppermute(value, "c", [(0, 1), (1, 0)])


def gather_along_z(own):
    half = 40
    up2, down2 = along_z(own, 2), along_z(own, -2)
    up1, down1 = along_z(own, 1), along_z(own, -1)
    up3, down3 = along_z(up2, 1), along_z(down2, -1)
    far_a, far_b = along_z(up2[:half], 2), along_z(down2[half:], -2)
    pieces = (own, down1, down2, down3, far_a, far_b, up3, up2, up1)
    return call(
        join_kernel, "join", pieces, struct((8 * PIECE, own.shape[1]), jnp.bfloat16), VMEM, limit=8
    )


def rolled(row, z, sign):
    for bit in (1, 2, 4):
        turned = pltpu.roll(row, (sign * bit * ROWS) % 512, 1)
        row = jnp.where((z & bit) != 0, turned, row)
    return row


def place():
    z = lax.axis_index("zh") * 2 + lax.axis_index("zl")
    return z, lax.axis_index("c")


def to_absolute(row, z, c):
    mine, other = rolled(row[:, :512], z, 1), rolled(row[:, 512:], z, 1)
    first = jnp.where(c == 0, mine, other)
    second = jnp.where(c == 0, other, mine)
    return jnp.concatenate([first, second], axis=1)


def to_relative(row, z, c):
    first, second = row[:, :512], row[:, 512:]
    mine = jnp.where(c == 0, first, second)
    other = jnp.where(c == 0, second, first)
    return jnp.concatenate([rolled(mine, z, -1), rolled(other, z, -1)], axis=1)


def prepare_kernel(q_in, p_in, positive_in, q_ref, p_ref, q_wide, p_wide, half_ref, index_ref, sems):
    loads = [
        pltpu.make_async_copy(p_in, p_wide, sems.at[16]),
        pltpu.make_async_copy(q_in, q_wide, sems.at[17]),
        pltpu.make_async_copy(positive_in, index_ref, sems.at[18]),
    ]
    for load in loads:
        load.start()
    loads[0].wait()
    half_ref[...] = p_wide[...].astype(jnp.bfloat16)
    copies = [pltpu.make_async_copy(half_ref, p_ref.at[i], sems.at[i]) for i in range(16)]
    for copy in copies:
        copy.start()
    loads[1].wait()
    q_ref[:ROWS, :] = q_wide[...].astype(jnp.bfloat16)
    loads[2].wait()
    index = index_ref[...]
    index = jnp.concatenate([index] * 16, axis=1)
    row = lax.broadcasted_iota(jnp.int32, (PIECE - ROWS, BLOCK), 0)
    meta = jnp.where(row == 0, index >> 7, jnp.where(row == 1, index & 127, 0))
    q_ref[ROWS:, :] = meta.astype(jnp.float32).astype(jnp.bfloat16)
    for copy in copies:
        copy.wait()


def join_kernel(*refs):
    out_ref, at = refs[-1], 0
    for ref in refs[:-1]:
        rows = ref.shape[0]
        out_ref[at : at + rows, :] = ref[...]
        at += rows


def tile(k):
    return slice(k * TILE, (k + 1) * TILE)


def scores_kernel(own_ref, other_ref, p_in, q_ref, p_ref, target_ref, s_ref, stats_ref, sems):
    loads = [pltpu.make_async_copy(p_in.at[tile(j)], p_ref.at[tile(j)], sems.at[j]) for j in range(4)]
    for load in loads:
        load.start()
    z, c = place()
    lane_block = lax.broadcasted_iota(jnp.int32, (1, BLOCK), 1) // ROWS
    high = jnp.zeros((1, BLOCK), jnp.float32)
    low = jnp.zeros((1, BLOCK), jnp.float32)
    for slot in range(16):
        ref, at = (own_ref, slot * PIECE) if slot < 8 else (other_ref, (slot - 8) * PIECE)
        q_ref[slot * ROWS : (slot + 1) * ROWS, :] = ref[at : at + ROWS, :]
        meta = ref[at + ROWS : at + PIECE, :].astype(jnp.float32)
        high = jnp.where(lane_block == slot, meta[0:1], high)
        low = jnp.where(lane_block == slot, meta[1:2], low)
    target = high.astype(jnp.int32) * 128 + low.astype(jnp.int32)
    here = (
        (((target >> 6) & 3) == lax.axis_index("zh"))
        & (((target >> 8) & 1) == c)
        & (((target >> 11) & 1) == lax.axis_index("zl"))
    )
    column = ((target >> 12) & 3) * 256 + ((target >> 9) & 3) * 64 + (target & 63)
    target_ref[...] = jnp.where(here, column, -1)

    lse, positive = [], []
    for i in range(4):
        column = target_ref[:, tile(i)]
        highest = jnp.full((1, TILE), -jnp.inf, jnp.float32)
        pos = jnp.zeros((1, TILE), jnp.float32)
        for j in range(4):
            if i == 0:
                loads[j].wait()
            s = logit_scale * lax.dot_general(
                p_ref[tile(j), :], q_ref[tile(i), :], (((1,), (1,)), ((), ())),
                preferred_element_type=jnp.float32,
            )
            s_ref[tile(j), tile(i)] = s
            row = lax.broadcasted_iota(jnp.int32, (TILE, TILE), 0) + j * TILE
            pos = pos + jnp.sum(jnp.where(row == column, s, 0.0), axis=0, keepdims=True)
            highest = jnp.maximum(highest, jnp.max(s, axis=0, keepdims=True))
        acc = jnp.zeros((1, TILE), jnp.float32)
        for j in range(4):
            acc = acc + jnp.sum(jnp.exp(s_ref[tile(j), tile(i)] - highest), axis=0, keepdims=True)
        lse.append(highest + jnp.log(acc))
        positive.append(pos)
    for at, parts in ((0, lse), (8, positive)):
        row = to_absolute(jnp.concatenate(parts, axis=1), z, c)
        for r in range(8):
            stats_ref[0, at + r : at + r + 1, :] = row[:, r * 128 : (r + 1) * 128]
    for k in range(1, 16):
        stats_ref[k] = stats_ref[0]


def weights_kernel(
    stats_ref, target_ref, s_ref, q_ref, p_ref, out_ref, mine_ref, other_ref, loss_ref,
    w_ref, terms_ref, sums_ref, sems,
):
    z, c = place()
    stats = stats_ref[...]
    lses = stats[:, 0:8, :]
    highest = jnp.max(lses, axis=0)
    log_norm = highest + jnp.log(jnp.sum(jnp.exp(lses - highest[None]), axis=0))
    positive = jnp.sum(stats[:, 8:16, :], axis=0)
    log_norm, positive = (
        to_relative(jnp.concatenate([v[r : r + 1] for r in range(8)], axis=1), z, c)
        for v in (log_norm, positive)
    )
    loss_ref[...] = (log_norm - positive)[:, 0:ROWS]
    stores = []
    for j in range(4):
        for i in range(4):
            row = lax.broadcasted_iota(jnp.int32, (TILE, TILE), 0) + j * TILE
            onehot = jnp.where(row == target_ref[:, tile(i)], 1.0, 0.0)
            w = (jnp.exp(s_ref[tile(j), tile(i)] - log_norm[:, tile(i)]) - onehot) * logit_scale
            w_ref[tile(j), tile(i)] = w.astype(jnp.bfloat16)
        for k in range(4):
            terms_ref[tile(j), tile(k)] = jnp.dot(
                w_ref[tile(j), :], q_ref[:, tile(k)], preferred_element_type=jnp.float32
            ).astype(jnp.bfloat16)
        stores.append(pltpu.make_async_copy(terms_ref.at[tile(j)], out_ref.at[tile(j)], sems.at[j]))
        stores[-1].start()
    for i in range(4):
        for k in range(4):
            product = lax.dot_general(
                w_ref[:, tile(i)], p_ref[:, tile(k)], (((0,), (0,)), ((), ())),
                preferred_element_type=jnp.float32,
            )
            if i >= 2:
                other_ref[tile(i - 2), tile(k)] = product
            else:
                sums_ref[tile(i), tile(k)] = product
        if i < 2:
            stores.append(
                pltpu.make_async_copy(sums_ref.at[tile(i)], mine_ref.at[tile(i)], sems.at[4 + i])
            )
            stores[-1].start()
    for store in stores:
        store.wait()


def split_kernel(mine_in, arrived_ref, own_ref, *rest):
    outs, mine_ref, sems = rest[:7], rest[7], rest[8]
    rows = [slice(slot * ROWS, (slot + 1) * ROWS) for slot in range(8)]
    loads = [pltpu.make_async_copy(mine_in.at[r], mine_ref.at[r], sems.at[i]) for i, r in enumerate(rows)]
    for load in loads:
        load.start()
    for slot, at in enumerate(rows):
        loads[slot].wait()
        total = mine_ref[at, :] + arrived_ref[at, :]
        if slot == 0:
            own_ref[...] = total
        else:
            outs[slot - 1][...] = total.astype(jnp.bfloat16)


def total_kernel(p_in, own_ref, *rest):
    pieces, (q_out, p_out), (p_ref, sum_ref, sems) = rest[:7], rest[7:9], rest[9:]
    loads = [pltpu.make_async_copy(p_in.at[i], p_ref.at[i], sems.at[i]) for i in range(16)]
    for load in loads:
        load.start()
    total = own_ref[...]
    for piece in pieces:
        total = total + piece[...].astype(jnp.float32)
    sum_ref[0] = total
    store = pltpu.make_async_copy(sum_ref.at[0], q_out, sems.at[16])
    store.start()
    for load in loads:
        load.wait()
    total = p_ref[0].astype(jnp.float32)
    for i in range(1, 16):
        total = total + p_ref[i].astype(jnp.float32)
    sum_ref[1] = total
    last = pltpu.make_async_copy(sum_ref.at[1], p_out, sems.at[17])
    last.start()
    store.wait()
    last.wait()


def cost(flops, count):
    return pl.CostEstimate(flops=flops, bytes_accessed=count, transcendentals=0)


def struct(shape, dtype):
    return jax.ShapeDtypeStruct(shape, dtype)


def far(shape, dtype):
    return pltpu.HBM(shape, dtype)


def call(kernel, name, args, out_shape, out_specs, limit, flops=1 << 28, scratch=(), held=()):
    return pl.pallas_call(
        kernel,
        out_shape=out_shape,
        in_specs=[HBM if i in held else VMEM for i in range(len(args))],
        out_specs=out_specs,
        scratch_shapes=scratch,
        compiler_params=pltpu.CompilerParams(vmem_limit_bytes=limit << 20),
        cost_estimate=cost(flops, 4 << 20),
        name=name,
    )(*(pltpu.with_memory_space_constraint(a, pltpu.HBM) if i in held else a for i, a in enumerate(args)))


def body(queries, passages, positives):
    width = queries.shape[1]
    matmul = 2 * BLOCK**3
    own, p_sent = call(
        prepare_kernel,
        "prepare",
        (queries, passages, positives.reshape(1, ROWS)),
        (struct((PIECE, width), jnp.bfloat16), far((16, ROWS, width), jnp.bfloat16)),
        (VMEM, HBM),
        limit=4,
        scratch=(
            pltpu.VMEM((ROWS, width), jnp.float32),
            pltpu.VMEM((ROWS, width), jnp.float32),
            pltpu.VMEM((ROWS, width), jnp.bfloat16),
            pltpu.VMEM((1, ROWS), jnp.int32),
            pltpu.SemaphoreType.DMA((19,)),
        ),
        held=(0, 1, 2),
    )
    p_block = lax.all_to_all(p_sent, XY, 0, 0, tiled=True).reshape(BLOCK, width)
    gathered = gather_along_z(own)
    partner = to_partner(gathered)
    q_block, p_block, column, scores, stats = call(
        scores_kernel,
        "scores",
        (gathered, partner, p_block),
        (
            struct((BLOCK, width), jnp.bfloat16),
            struct((BLOCK, width), jnp.bfloat16),
            struct((1, BLOCK), jnp.int32),
            struct((BLOCK, BLOCK), jnp.float32),
            struct((16, 16, 128), jnp.float32),
        ),
        (VMEM,) * 5,
        limit=20,
        flops=matmul,
        scratch=(pltpu.SemaphoreType.DMA((4,)),),
        held=(2,),
    )
    stats = lax.all_to_all(stats, ZC, 0, 0, tiled=True)
    half = (BLOCK // 2, width)
    p_terms, mine, others, losses = call(
        weights_kernel,
        "weights",
        (stats, column, scores, q_block, p_block),
        (
            far((BLOCK, width), jnp.bfloat16),
            far(half, jnp.float32),
            struct(half, jnp.float32),
            struct((1, ROWS), jnp.float32),
        ),
        (HBM, HBM, VMEM, VMEM),
        limit=30,
        flops=2 * matmul,
        scratch=(
            pltpu.VMEM((BLOCK, BLOCK), jnp.bfloat16),
            pltpu.VMEM((BLOCK, width), jnp.bfloat16),
            pltpu.VMEM(half, jnp.float32),
            pltpu.SemaphoreType.DMA((6,)),
        ),
    )
    p_terms = lax.all_to_all(p_terms.reshape(16, ROWS, width), XY, 0, 0, tiled=True)
    block = (ROWS, width)
    own_terms, *pieces = call(
        split_kernel,
        "split",
        (mine, to_partner(others)),
        (struct(block, jnp.float32),) + (struct(block, jnp.bfloat16),) * 7,
        (VMEM,) * 8,
        limit=8,
        scratch=(pltpu.VMEM(half, jnp.float32), pltpu.SemaphoreType.DMA((8,))),
        held=(0,),
    )
    arrived = [along_z(pieces[slot - 1], slot) for slot in (4, 5, 3, 6, 2, 7, 1)]
    query_grads, passage_grads = call(
        total_kernel,
        "total",
        (p_terms, own_terms, *arrived),
        (far(block, jnp.float32),) * 2,
        (HBM,) * 2,
        limit=8,
        scratch=(
            pltpu.VMEM((16, *block), jnp.bfloat16),
            pltpu.VMEM((2, *block), jnp.float32),
            pltpu.SemaphoreType.DMA((18,)),
        ),
        held=(0,),
    )
    return losses.reshape(ROWS), query_grads, passage_grads


def solution(mesh):
    torus = Mesh(mesh.devices.reshape(4, 2, 4, 2, 4), AXES)
    placed = (P(AXES, None), P(AXES, None), P(AXES))
    return jax.shard_map(
        body,
        mesh=torus,
        in_specs=placed,
        out_specs=(P(AXES), P(AXES, None), P(AXES, None)),
        check_vma=False,
    )
```

```python
import functools

import jax
import jax.numpy as jnp
import numpy as np
from jax import lax
from jax.experimental import pallas as pl
from jax.experimental.pallas import tpu as pltpu
from jax.sharding import Mesh
from jax.sharding import PartitionSpec as P

AXES = ("x", "zl", "y", "c", "zh")
SIZES = {"x": 4, "zl": 2, "y": 4, "c": 2, "zh": 4}
XY = ("x", "y")
ZC = ("c", "zh", "zl")

logit_scale = 20.0
ROWS = 64
BLOCK = 1024
TILE = 256
PIECE = 72
VMEM = pl.BlockSpec(memory_space=pltpu.VMEM)
HBM = pl.BlockSpec(memory_space=pltpu.HBM)


def along_z(value, shift):
    pairs = []
    for i in range(8):
        zl, zh = divmod(i, 4)
        to = (zh * 2 + zl + shift) % 8
        pairs.append((i, (to % 2) * 4 + to // 2))
    return lax.ppermute(value, ("zl", "zh"), pairs)


def to_partner(value):
    return lax.ppermute(value, "c", [(0, 1), (1, 0)])


def gather_along_z(own):
    half = 40
    up2, down2 = along_z(own, 2), along_z(own, -2)
    up1, down1 = along_z(own, 1), along_z(own, -1)
    up3, down3 = along_z(up2, 1), along_z(down2, -1)
    far_a, far_b = along_z(up2[:half], 2), along_z(down2[half:], -2)
    pieces = (own, down1, down2, down3, far_a, far_b, up3, up2, up1)
    return call(
        join_kernel, "join", pieces, struct((8 * PIECE, own.shape[1]), jnp.bfloat16), VMEM, limit=8
    )


def rolled(row, z, sign):
    for bit in (1, 2, 4):
        turned = pltpu.roll(row, (sign * bit * ROWS) % 512, 1)
        row = jnp.where((z & bit) != 0, turned, row)
    return row


def place():
    z = lax.axis_index("zh") * 2 + lax.axis_index("zl")
    return z, lax.axis_index("c")


def to_absolute(row, z, c):
    mine, other = rolled(row[:, :512], z, 1), rolled(row[:, 512:], z, 1)
    first = jnp.where(c == 0, mine, other)
    second = jnp.where(c == 0, other, mine)
    return jnp.concatenate([first, second], axis=1)


def to_relative(row, z, c):
    first, second = row[:, :512], row[:, 512:]
    mine = jnp.where(c == 0, first, second)
    other = jnp.where(c == 0, second, first)
    return jnp.concatenate([rolled(mine, z, -1), rolled(other, z, -1)], axis=1)


def prepare_kernel(q_in, p_in, positive_in, q_ref, p_ref, q_wide, p_wide, half_ref, index_ref, sems):
    loads = [
        pltpu.make_async_copy(p_in, p_wide, sems.at[16]),
        pltpu.make_async_copy(q_in, q_wide, sems.at[17]),
        pltpu.make_async_copy(positive_in, index_ref, sems.at[18]),
    ]
    for load in loads:
        load.start()
    loads[0].wait()
    half_ref[...] = p_wide[...].astype(jnp.bfloat16)
    copies = [pltpu.make_async_copy(half_ref, p_ref.at[i], sems.at[i]) for i in range(16)]
    for copy in copies:
        copy.start()
    loads[1].wait()
    q_ref[:ROWS, :] = q_wide[...].astype(jnp.bfloat16)
    loads[2].wait()
    index = index_ref[...]
    index = jnp.concatenate([index] * 16, axis=1)
    row = lax.broadcasted_iota(jnp.int32, (PIECE - ROWS, BLOCK), 0)
    meta = jnp.where(row == 0, index >> 7, jnp.where(row == 1, index & 127, 0))
    q_ref[ROWS:, :] = meta.astype(jnp.float32).astype(jnp.bfloat16)
    for copy in copies:
        copy.wait()


def join_kernel(*refs):
    out_ref, at = refs[-1], 0
    for ref in refs[:-1]:
        rows = ref.shape[0]
        out_ref[at : at + rows, :] = ref[...]
        at += rows


def tile(k):
    return slice(k * TILE, (k + 1) * TILE)


def take_queries(ref, q_ref, target_ref, half):
    lane_block = lax.broadcasted_iota(jnp.int32, (1, BLOCK // 2), 1) // ROWS
    high = jnp.zeros((1, BLOCK // 2), jnp.float32)
    low = jnp.zeros((1, BLOCK // 2), jnp.float32)
    for slot in range(8):
        at, to = slot * PIECE, half * (BLOCK // 2) + slot * ROWS
        q_ref[to : to + ROWS, :] = ref[at : at + ROWS, :]
        meta = ref[at + ROWS : at + PIECE, : BLOCK // 2].astype(jnp.float32)
        high = jnp.where(lane_block == slot, meta[0:1], high)
        low = jnp.where(lane_block == slot, meta[1:2], low)
    target = high.astype(jnp.int32) * 128 + low.astype(jnp.int32)
    here = (
        (((target >> 6) & 3) == lax.axis_index("zh"))
        & (((target >> 8) & 1) == lax.axis_index("c"))
        & (((target >> 11) & 1) == lax.axis_index("zl"))
    )
    column = ((target >> 12) & 3) * 256 + ((target >> 9) & 3) * 64 + (target & 63)
    target_ref[:, half * (BLOCK // 2) : (half + 1) * (BLOCK // 2)] = jnp.where(here, column, -1)


def scores_kernel(
    own_ref, other_in, p_ref, q_ref, target_ref, e_ref, highest_ref, stats_ref, other_ref, sem
):
    load = pltpu.make_async_copy(other_in, other_ref, sem)
    load.start()
    z, c = place()
    take_queries(own_ref, q_ref, target_ref, 0)
    lse, positive = [], []
    for i in range(4):
        if i == 2:
            load.wait()
            take_queries(other_ref, q_ref, target_ref, 1)
        column = target_ref[:, tile(i)]
        highest = jnp.full((1, TILE), -jnp.inf, jnp.float32)
        pos = jnp.zeros((1, TILE), jnp.float32)
        for j in range(4):
            s = logit_scale * lax.dot_general(
                p_ref[tile(j), :], q_ref[tile(i), :], (((1,), (1,)), ((), ())),
                preferred_element_type=jnp.float32,
            )
            e_ref[tile(j), tile(i)] = s
            row = lax.broadcasted_iota(jnp.int32, (TILE, TILE), 0) + j * TILE
            pos = pos + jnp.sum(jnp.where(row == column, s, 0.0), axis=0, keepdims=True)
            highest = jnp.maximum(highest, jnp.max(s, axis=0, keepdims=True))
        acc = jnp.zeros((1, TILE), jnp.float32)
        for j in range(4):
            e = jnp.exp(e_ref[tile(j), tile(i)] - highest)
            e_ref[tile(j), tile(i)] = e
            acc = acc + jnp.sum(e, axis=0, keepdims=True)
        highest_ref[:, tile(i)] = highest
        lse.append(highest + jnp.log(acc))
        positive.append(pos)
    for at, parts in ((0, lse), (8, positive)):
        row = to_absolute(jnp.concatenate(parts, axis=1), z, c)
        for r in range(8):
            stats_ref[0, at + r : at + r + 1, :] = row[:, r * 128 : (r + 1) * 128]
    for k in range(1, 16):
        stats_ref[k] = stats_ref[0]


def weights_kernel(
    stats_ref, target_ref, e_ref, highest_ref, q_ref, p_ref, out_ref, mine_ref, other_ref, loss_ref,
    w_ref, terms_ref, sums_ref, sems,
):
    z, c = place()
    stats = stats_ref[...]
    lses = stats[:, 0:8, :]
    highest = jnp.max(lses, axis=0)
    log_norm = highest + jnp.log(jnp.sum(jnp.exp(lses - highest[None]), axis=0))
    positive = jnp.sum(stats[:, 8:16, :], axis=0)
    log_norm, positive = (
        to_relative(jnp.concatenate([v[r : r + 1] for r in range(8)], axis=1), z, c)
        for v in (log_norm, positive)
    )
    loss_ref[...] = (log_norm - positive)[:, 0:ROWS]
    factor = logit_scale * jnp.exp(highest_ref[...] - log_norm)
    stores = []
    for j in range(4):
        for i in range(4):
            row = lax.broadcasted_iota(jnp.int32, (TILE, TILE), 0) + j * TILE
            taken = jnp.where(row == target_ref[:, tile(i)], logit_scale, 0.0)
            w = e_ref[tile(j), tile(i)] * factor[:, tile(i)] - taken
            w_ref[tile(j), tile(i)] = w.astype(jnp.bfloat16)
        for k in range(4):
            terms_ref[tile(j), tile(k)] = jnp.dot(
                w_ref[tile(j), :], q_ref[:, tile(k)], preferred_element_type=jnp.float32
            ).astype(jnp.bfloat16)
        stores.append(pltpu.make_async_copy(terms_ref.at[tile(j)], out_ref.at[tile(j)], sems.at[j]))
        stores[-1].start()
    for step, i in enumerate((2, 3, 0, 1)):
        for k in range(4):
            sums_ref[tile(i), tile(k)] = lax.dot_general(
                w_ref[:, tile(i)], p_ref[:, tile(k)], (((0,), (0,)), ((), ())),
                preferred_element_type=jnp.float32,
            )
        to_ref = mine_ref if i < 2 else other_ref
        stores.append(
            pltpu.make_async_copy(sums_ref.at[tile(i)], to_ref.at[tile(i % 2)], sems.at[4 + step])
        )
        stores[-1].start()
    for store in stores:
        store.wait()


def split_kernel(mine_in, arrived_ref, own_ref, *rest):
    outs, mine_ref, sems = rest[:7], rest[7], rest[8]
    rows = [slice(slot * ROWS, (slot + 1) * ROWS) for slot in range(8)]
    loads = [pltpu.make_async_copy(mine_in.at[r], mine_ref.at[r], sems.at[i]) for i, r in enumerate(rows)]
    for load in loads:
        load.start()
    for slot, at in enumerate(rows):
        loads[slot].wait()
        total = mine_ref[at, :] + arrived_ref[at, :]
        if slot == 0:
            own_ref[...] = total
        else:
            outs[slot - 1][...] = total.astype(jnp.bfloat16)


def total_kernel(p_in, own_ref, *rest):
    pieces, (q_out, p_out), (p_ref, sum_ref, sems) = rest[:7], rest[7:9], rest[9:]
    rows = [slice(k * 16, (k + 1) * 16) for k in range(4)]
    loads = [pltpu.make_async_copy(p_in.at[:, r], p_ref.at[:, r], sems.at[k]) for k, r in enumerate(rows)]
    for load in loads:
        load.start()
    total = own_ref[...]
    for piece in pieces:
        total = total + piece[...].astype(jnp.float32)
    sum_ref[0] = total
    stores = [pltpu.make_async_copy(sum_ref.at[0], q_out, sems.at[4])]
    stores[0].start()
    for k, r in enumerate(rows):
        loads[k].wait()
        total = p_ref[0, r, :].astype(jnp.float32)
        for i in range(1, 16):
            total = total + p_ref[i, r, :].astype(jnp.float32)
        sum_ref[1, r, :] = total
        stores.append(pltpu.make_async_copy(sum_ref.at[1, r], p_out.at[r], sems.at[5 + k]))
        stores[-1].start()
    for store in stores:
        store.wait()


def cost(flops, count):
    return pl.CostEstimate(flops=flops, bytes_accessed=count, transcendentals=0)


def struct(shape, dtype):
    return jax.ShapeDtypeStruct(shape, dtype)


def far(shape, dtype):
    return pltpu.HBM(shape, dtype)


def call(kernel, name, args, out_shape, out_specs, limit, flops=1 << 28, scratch=(), held=()):
    return pl.pallas_call(
        kernel,
        out_shape=out_shape,
        in_specs=[HBM if i in held else VMEM for i in range(len(args))],
        out_specs=out_specs,
        scratch_shapes=scratch,
        compiler_params=pltpu.CompilerParams(vmem_limit_bytes=limit << 20),
        cost_estimate=cost(flops, 4 << 20),
        name=name,
    )(*(pltpu.with_memory_space_constraint(a, pltpu.HBM) if i in held else a for i, a in enumerate(args)))


def body(queries, passages, positives):
    width = queries.shape[1]
    matmul = 2 * BLOCK**3
    own, p_sent = call(
        prepare_kernel,
        "prepare",
        (queries, passages, positives.reshape(1, ROWS)),
        (struct((PIECE, width), jnp.bfloat16), far((16, ROWS, width), jnp.bfloat16)),
        (VMEM, HBM),
        limit=4,
        scratch=(
            pltpu.VMEM((ROWS, width), jnp.float32),
            pltpu.VMEM((ROWS, width), jnp.float32),
            pltpu.VMEM((ROWS, width), jnp.bfloat16),
            pltpu.VMEM((1, ROWS), jnp.int32),
            pltpu.SemaphoreType.DMA((19,)),
        ),
        held=(0, 1, 2),
    )
    p_block = lax.all_to_all(p_sent, XY, 0, 0, tiled=True).reshape(BLOCK, width)
    gathered = gather_along_z(own)
    partner = to_partner(gathered)
    q_block, column, scores, highest, stats = call(
        scores_kernel,
        "scores",
        (gathered, partner, p_block),
        (
            struct((BLOCK, width), jnp.bfloat16),
            struct((1, BLOCK), jnp.int32),
            struct((BLOCK, BLOCK), jnp.float32),
            struct((1, BLOCK), jnp.float32),
            struct((16, 16, 128), jnp.float32),
        ),
        (VMEM,) * 5,
        limit=20,
        flops=matmul,
        scratch=(pltpu.VMEM((8 * PIECE, width), jnp.bfloat16), pltpu.SemaphoreType.DMA),
        held=(1,),
    )
    stats = lax.all_to_all(stats, ZC, 0, 0, tiled=True)
    half = (BLOCK // 2, width)
    p_terms, mine, others, losses = call(
        weights_kernel,
        "weights",
        (stats, column, scores, highest, q_block, p_block),
        (
            far((BLOCK, width), jnp.bfloat16),
            far(half, jnp.float32),
            far(half, jnp.float32),
            struct((1, ROWS), jnp.float32),
        ),
        (HBM, HBM, HBM, VMEM),
        limit=30,
        flops=2 * matmul,
        scratch=(
            pltpu.VMEM((BLOCK, BLOCK), jnp.bfloat16),
            pltpu.VMEM((BLOCK, width), jnp.bfloat16),
            pltpu.VMEM((BLOCK, width), jnp.float32),
            pltpu.SemaphoreType.DMA((8,)),
        ),
    )
    p_terms = lax.all_to_all(p_terms.reshape(16, ROWS, width), XY, 0, 0, tiled=True)
    block = (ROWS, width)
    own_terms, *pieces = call(
        split_kernel,
        "split",
        (mine, to_partner(others)),
        (struct(block, jnp.float32),) + (struct(block, jnp.bfloat16),) * 7,
        (VMEM,) * 8,
        limit=8,
        scratch=(pltpu.VMEM(half, jnp.float32), pltpu.SemaphoreType.DMA((8,))),
        held=(0,),
    )
    arrived = [along_z(pieces[slot - 1], slot) for slot in (4, 5, 3, 6, 2, 7, 1)]
    query_grads, passage_grads = call(
        total_kernel,
        "total",
        (p_terms, own_terms, *arrived),
        (far(block, jnp.float32),) * 2,
        (HBM,) * 2,
        limit=8,
        scratch=(
            pltpu.VMEM((16, *block), jnp.bfloat16),
            pltpu.VMEM((2, *block), jnp.float32),
            pltpu.SemaphoreType.DMA((9,)),
        ),
        held=(0,),
    )
    return losses.reshape(ROWS), query_grads, passage_grads


def solution(mesh):
    torus = Mesh(mesh.devices.reshape(4, 2, 4, 2, 4), AXES)
    placed = (P(AXES, None), P(AXES, None), P(AXES))
    return jax.shard_map(
        body,
        mesh=torus,
        in_specs=placed,
        out_specs=(P(AXES), P(AXES, None), P(AXES, None)),
        check_vma=False,
    )
```

```python
import functools

import jax
import jax.numpy as jnp
import numpy as np
from jax import lax
from jax.experimental import pallas as pl
from jax.experimental.pallas import tpu as pltpu
from jax.sharding import Mesh
from jax.sharding import PartitionSpec as P

AXES = ("x", "zl", "y", "c", "za", "zb")
XY = ("x", "y")
ZC = ("zl", "zb", "za", "c")

logit_scale = 20.0
ROWS = 64
BLOCK = 1024
TILE = 256
PIECE = 72
VMEM = pl.BlockSpec(memory_space=pltpu.VMEM)
HBM = pl.BlockSpec(memory_space=pltpu.HBM)


def along_z(value, shift):
    pairs = []
    for i in range(8):
        zl, zh = divmod(i, 4)
        to = (zh * 2 + zl + shift) % 8
        pairs.append((i, (to % 2) * 4 + to // 2))
    return lax.ppermute(value, ("zl", "za", "zb"), pairs)


def to_partner(value):
    return lax.ppermute(value, "c", [(0, 1), (1, 0)])


def gather_along_z(own):
    half = 40
    up2, down2 = along_z(own, 2), along_z(own, -2)
    up1, down1 = along_z(own, 1), along_z(own, -1)
    up3, down3 = along_z(up2, 1), along_z(down2, -1)
    far_a, far_b = along_z(up2[:half], 2), along_z(down2[half:], -2)
    pieces = (own, down1, down2, down3, far_a, far_b, up3, up2, up1)
    return call(
        join_kernel, "join", pieces, struct((8 * PIECE, own.shape[1]), jnp.bfloat16), VMEM, limit=8
    )


def rolled(row, z, sign):
    for bit in (1, 2, 4):
        turned = pltpu.roll(row, (sign * bit * ROWS) % 512, 1)
        row = jnp.where((z & bit) != 0, turned, row)
    return row


def high_z():
    return lax.axis_index("za") * 2 + lax.axis_index("zb")


def place():
    z = high_z() * 2 + lax.axis_index("zl")
    return z, lax.axis_index("c")


def to_absolute(row, z, c):
    mine, other = rolled(row[:, :512], z, 1), rolled(row[:, 512:], z, 1)
    first = jnp.where(c == 0, mine, other)
    second = jnp.where(c == 0, other, mine)
    return jnp.concatenate([first, second], axis=1)


def to_relative(row, z, c):
    first, second = row[:, :512], row[:, 512:]
    mine = jnp.where(c == 0, first, second)
    other = jnp.where(c == 0, second, first)
    return jnp.concatenate([rolled(mine, z, -1), rolled(other, z, -1)], axis=1)


def prepare_kernel(q_in, p_in, positive_in, q_ref, p_ref, q_wide, p_wide, half_ref, index_ref, sems):
    loads = [
        pltpu.make_async_copy(p_in, p_wide, sems.at[16]),
        pltpu.make_async_copy(q_in, q_wide, sems.at[17]),
        pltpu.make_async_copy(positive_in, index_ref, sems.at[18]),
    ]
    for load in loads:
        load.start()
    loads[0].wait()
    half_ref[...] = p_wide[...].astype(jnp.bfloat16)
    copies = [pltpu.make_async_copy(half_ref, p_ref.at[i], sems.at[i]) for i in range(16)]
    for copy in copies:
        copy.start()
    loads[1].wait()
    q_ref[:ROWS, :] = q_wide[...].astype(jnp.bfloat16)
    loads[2].wait()
    index = index_ref[...]
    index = jnp.concatenate([index] * 16, axis=1)
    row = lax.broadcasted_iota(jnp.int32, (PIECE - ROWS, BLOCK), 0)
    meta = jnp.where(row == 0, index >> 7, jnp.where(row == 1, index & 127, 0))
    q_ref[ROWS:, :] = meta.astype(jnp.float32).astype(jnp.bfloat16)
    for copy in copies:
        copy.wait()


def join_kernel(*refs):
    out_ref, at = refs[-1], 0
    for ref in refs[:-1]:
        rows = ref.shape[0]
        out_ref[at : at + rows, :] = ref[...]
        at += rows


def tile(k):
    return slice(k * TILE, (k + 1) * TILE)


def take_queries(ref, q_ref, target_ref, half):
    lane_block = lax.broadcasted_iota(jnp.int32, (1, BLOCK // 2), 1) // ROWS
    high = jnp.zeros((1, BLOCK // 2), jnp.float32)
    low = jnp.zeros((1, BLOCK // 2), jnp.float32)
    for slot in range(8):
        at, to = slot * PIECE, half * (BLOCK // 2) + slot * ROWS
        q_ref[to : to + ROWS, :] = ref[at : at + ROWS, :]
        meta = ref[at + ROWS : at + PIECE, : BLOCK // 2].astype(jnp.float32)
        high = jnp.where(lane_block == slot, meta[0:1], high)
        low = jnp.where(lane_block == slot, meta[1:2], low)
    target = high.astype(jnp.int32) * 128 + low.astype(jnp.int32)
    here = (
        (((target >> 6) & 3) == high_z())
        & (((target >> 8) & 1) == lax.axis_index("c"))
        & (((target >> 11) & 1) == lax.axis_index("zl"))
    )
    column = ((target >> 12) & 3) * 256 + ((target >> 9) & 3) * 64 + (target & 63)
    target_ref[:, half * (BLOCK // 2) : (half + 1) * (BLOCK // 2)] = jnp.where(here, column, -1)


def scores_kernel(
    own_ref, other_in, p_ref, q_ref, target_ref, e_ref, highest_ref, stats_ref, other_ref, sem
):
    load = pltpu.make_async_copy(other_in, other_ref, sem)
    load.start()
    z, c = place()
    take_queries(own_ref, q_ref, target_ref, 0)
    lse, positive = [], []
    for i in range(4):
        if i == 2:
            load.wait()
            take_queries(other_ref, q_ref, target_ref, 1)
        column = target_ref[:, tile(i)]
        highest = jnp.full((1, TILE), -jnp.inf, jnp.float32)
        pos = jnp.zeros((1, TILE), jnp.float32)
        for j in range(4):
            s = logit_scale * lax.dot_general(
                p_ref[tile(j), :], q_ref[tile(i), :], (((1,), (1,)), ((), ())),
                preferred_element_type=jnp.float32,
            )
            e_ref[tile(j), tile(i)] = s
            row = lax.broadcasted_iota(jnp.int32, (TILE, TILE), 0) + j * TILE
            pos = pos + jnp.sum(jnp.where(row == column, s, 0.0), axis=0, keepdims=True)
            highest = jnp.maximum(highest, jnp.max(s, axis=0, keepdims=True))
        acc = jnp.zeros((1, TILE), jnp.float32)
        for j in range(4):
            e = jnp.exp(e_ref[tile(j), tile(i)] - highest)
            e_ref[tile(j), tile(i)] = e
            acc = acc + jnp.sum(e, axis=0, keepdims=True)
        highest_ref[:, tile(i)] = highest
        lse.append(highest + jnp.log(acc))
        positive.append(pos)
    for at, parts in ((0, lse), (8, positive)):
        row = to_absolute(jnp.concatenate(parts, axis=1), z, c)
        for r in range(8):
            stats_ref[0, at + r : at + r + 1, :] = row[:, r * 128 : (r + 1) * 128]
    for k in range(1, 16):
        stats_ref[k] = stats_ref[0]


def weights_kernel(
    stats_ref, target_ref, e_ref, highest_ref, q_ref, p_ref, out_ref, mine_ref, other_ref, loss_ref,
    w_ref, terms_ref, sums_ref, sems,
):
    z, c = place()
    stats = stats_ref[...]
    lses = stats[:, 0:8, :]
    highest = jnp.max(lses, axis=0)
    log_norm = highest + jnp.log(jnp.sum(jnp.exp(lses - highest[None]), axis=0))
    positive = jnp.sum(stats[:, 8:16, :], axis=0)
    log_norm, positive = (
        to_relative(jnp.concatenate([v[r : r + 1] for r in range(8)], axis=1), z, c)
        for v in (log_norm, positive)
    )
    loss_ref[...] = (log_norm - positive)[:, 0:ROWS]
    factor = logit_scale * jnp.exp(highest_ref[...] - log_norm)
    stores = []
    for j in range(4):
        for i in range(4):
            row = lax.broadcasted_iota(jnp.int32, (TILE, TILE), 0) + j * TILE
            taken = jnp.where(row == target_ref[:, tile(i)], logit_scale, 0.0)
            w = e_ref[tile(j), tile(i)] * factor[:, tile(i)] - taken
            w_ref[tile(j), tile(i)] = w.astype(jnp.bfloat16)
        for k in range(4):
            terms_ref[tile(j), tile(k)] = jnp.dot(
                w_ref[tile(j), :], q_ref[:, tile(k)], preferred_element_type=jnp.float32
            ).astype(jnp.bfloat16)
        stores.append(pltpu.make_async_copy(terms_ref.at[tile(j)], out_ref.at[tile(j)], sems.at[j]))
        stores[-1].start()
    for step, i in enumerate((2, 3, 0, 1)):
        for k in range(4):
            sums_ref[tile(i), tile(k)] = lax.dot_general(
                w_ref[:, tile(i)], p_ref[:, tile(k)], (((0,), (0,)), ((), ())),
                preferred_element_type=jnp.float32,
            )
        to_ref = mine_ref if i < 2 else other_ref
        stores.append(
            pltpu.make_async_copy(sums_ref.at[tile(i)], to_ref.at[tile(i % 2)], sems.at[4 + step])
        )
        stores[-1].start()
    for store in stores:
        store.wait()


def split_kernel(mine_in, arrived_ref, own_ref, *rest):
    outs, mine_ref, sems = rest[:7], rest[7], rest[8]
    rows = [slice(slot * ROWS, (slot + 1) * ROWS) for slot in range(8)]
    loads = [pltpu.make_async_copy(mine_in.at[r], mine_ref.at[r], sems.at[i]) for i, r in enumerate(rows)]
    for load in loads:
        load.start()
    for slot, at in enumerate(rows):
        loads[slot].wait()
        total = mine_ref[at, :] + arrived_ref[at, :]
        if slot == 0:
            own_ref[...] = total
        else:
            outs[slot - 1][...] = total.astype(jnp.bfloat16)


def total_kernel(p_ref, own_ref, *rest):
    pieces, (q_out, p_out), (sum_ref, sems) = rest[:7], rest[7:9], rest[9:]
    stores = []
    for k in range(4):
        r = slice(k * 16, (k + 1) * 16)
        total = p_ref[0, r, :].astype(jnp.float32)
        for i in range(1, 16):
            total = total + p_ref[i, r, :].astype(jnp.float32)
        sum_ref[1, r, :] = total
        stores.append(pltpu.make_async_copy(sum_ref.at[1, r], p_out.at[r], sems.at[k]))
        stores[-1].start()
    total = own_ref[...]
    for piece in pieces:
        total = total + piece[...].astype(jnp.float32)
    sum_ref[0] = total
    stores.append(pltpu.make_async_copy(sum_ref.at[0], q_out, sems.at[4]))
    stores[-1].start()
    for store in stores:
        store.wait()


def cost(flops, count):
    return pl.CostEstimate(flops=flops, bytes_accessed=count, transcendentals=0)


def struct(shape, dtype):
    return jax.ShapeDtypeStruct(shape, dtype)


def far(shape, dtype):
    return pltpu.HBM(shape, dtype)


def call(kernel, name, args, out_shape, out_specs, limit, flops=1 << 28, scratch=(), held=()):
    return pl.pallas_call(
        kernel,
        out_shape=out_shape,
        in_specs=[HBM if i in held else VMEM for i in range(len(args))],
        out_specs=out_specs,
        scratch_shapes=scratch,
        compiler_params=pltpu.CompilerParams(vmem_limit_bytes=limit << 20),
        cost_estimate=cost(flops, 4 << 20),
        name=name,
    )(*(pltpu.with_memory_space_constraint(a, pltpu.HBM) if i in held else a for i, a in enumerate(args)))


def body(queries, passages, positives):
    width = queries.shape[1]
    matmul = 2 * BLOCK**3
    own, p_sent = call(
        prepare_kernel,
        "prepare",
        (queries, passages, positives.reshape(1, ROWS)),
        (struct((PIECE, width), jnp.bfloat16), far((16, ROWS, width), jnp.bfloat16)),
        (VMEM, HBM),
        limit=4,
        scratch=(
            pltpu.VMEM((ROWS, width), jnp.float32),
            pltpu.VMEM((ROWS, width), jnp.float32),
            pltpu.VMEM((ROWS, width), jnp.bfloat16),
            pltpu.VMEM((1, ROWS), jnp.int32),
            pltpu.SemaphoreType.DMA((19,)),
        ),
        held=(0, 1, 2),
    )
    p_block = lax.all_to_all(p_sent, XY, 0, 0, tiled=True).reshape(BLOCK, width)
    gathered = gather_along_z(own)
    partner = to_partner(gathered)
    q_block, column, scores, highest, stats = call(
        scores_kernel,
        "scores",
        (gathered, partner, p_block),
        (
            struct((BLOCK, width), jnp.bfloat16),
            struct((1, BLOCK), jnp.int32),
            struct((BLOCK, BLOCK), jnp.float32),
            struct((1, BLOCK), jnp.float32),
            struct((16, 16, 128), jnp.float32),
        ),
        (VMEM,) * 5,
        limit=20,
        flops=matmul,
        scratch=(pltpu.VMEM((8 * PIECE, width), jnp.bfloat16), pltpu.SemaphoreType.DMA),
        held=(1,),
    )
    stats = lax.all_to_all(stats, ZC, 0, 0, tiled=True)
    half = (BLOCK // 2, width)
    p_terms, mine, others, losses = call(
        weights_kernel,
        "weights",
        (stats, column, scores, highest, q_block, p_block),
        (
            far((BLOCK, width), jnp.bfloat16),
            far(half, jnp.float32),
            far(half, jnp.float32),
            struct((1, ROWS), jnp.float32),
        ),
        (HBM, HBM, HBM, VMEM),
        limit=30,
        flops=2 * matmul,
        scratch=(
            pltpu.VMEM((BLOCK, BLOCK), jnp.bfloat16),
            pltpu.VMEM((BLOCK, width), jnp.bfloat16),
            pltpu.VMEM((BLOCK, width), jnp.float32),
            pltpu.SemaphoreType.DMA((8,)),
        ),
    )
    p_terms = lax.all_to_all(p_terms.reshape(16, ROWS, width), XY, 0, 0, tiled=True)
    block = (ROWS, width)
    own_terms, *pieces = call(
        split_kernel,
        "split",
        (mine, to_partner(others)),
        (struct(block, jnp.float32),) + (struct(block, jnp.bfloat16),) * 7,
        (VMEM,) * 8,
        limit=8,
        scratch=(pltpu.VMEM(half, jnp.float32), pltpu.SemaphoreType.DMA((8,))),
        held=(0,),
    )
    arrived = [along_z(pieces[slot - 1], slot) for slot in (4, 5, 3, 6, 2, 7, 1)]
    query_grads, passage_grads = call(
        total_kernel,
        "total",
        (p_terms, own_terms, *arrived),
        (far(block, jnp.float32),) * 2,
        (HBM,) * 2,
        limit=8,
        scratch=(
            pltpu.VMEM((2, *block), jnp.float32),
            pltpu.SemaphoreType.DMA((5,)),
        ),
    )
    return losses.reshape(ROWS), query_grads, passage_grads


def solution(mesh):
    torus = Mesh(mesh.devices.reshape(4, 2, 4, 2, 2, 2), AXES)
    placed = (P(AXES, None), P(AXES, None), P(AXES))
    return jax.shard_map(
        body,
        mesh=torus,
        in_specs=placed,
        out_specs=(P(AXES), P(AXES, None), P(AXES, None)),
        check_vma=False,
    )
```

```python
import functools

import jax
import jax.numpy as jnp
import numpy as np
from jax import lax
from jax.experimental import pallas as pl
from jax.experimental.pallas import tpu as pltpu
from jax.sharding import Mesh
from jax.sharding import PartitionSpec as P

AXES = ("x", "zl", "y", "c", "za", "zb")
XY = ("x", "y")
ZC = ("zl", "zb", "za", "c")

logit_scale = 20.0
ROWS = 64
BLOCK = 1024
TILE = 256
PIECE = 72
VMEM = pl.BlockSpec(memory_space=pltpu.VMEM)
HBM = pl.BlockSpec(memory_space=pltpu.HBM)


def along_z(value, shift):
    pairs = []
    for i in range(8):
        zl, zh = divmod(i, 4)
        to = (zh * 2 + zl + shift) % 8
        pairs.append((i, (to % 2) * 4 + to // 2))
    return lax.ppermute(value, ("zl", "za", "zb"), pairs)


def to_partner(value):
    return lax.ppermute(value, "c", [(0, 1), (1, 0)])


def gather_along_z(own):
    half = 40
    up2, down2 = along_z(own, 2), along_z(own, -2)
    up1, down1 = along_z(own, 1), along_z(own, -1)
    up3, down3 = along_z(up2, 1), along_z(down2, -1)
    far_a, far_b = along_z(up2[:half], 2), along_z(down2[half:], -2)
    pieces = (own, down1, down2, down3, far_a, far_b, up3, up2, up1)
    return call(
        join_kernel, "join", pieces, struct((8 * PIECE, own.shape[1]), jnp.bfloat16), VMEM, limit=8
    )


def rolled(row, z, sign):
    for bit in (1, 2, 4):
        turned = pltpu.roll(row, (sign * bit * ROWS) % 512, 1)
        row = jnp.where((z & bit) != 0, turned, row)
    return row


def high_z():
    return lax.axis_index("za") * 2 + lax.axis_index("zb")


def place():
    z = high_z() * 2 + lax.axis_index("zl")
    return z, lax.axis_index("c")


def to_absolute(row, z, c):
    mine, other = rolled(row[:, :512], z, 1), rolled(row[:, 512:], z, 1)
    first = jnp.where(c == 0, mine, other)
    second = jnp.where(c == 0, other, mine)
    return jnp.concatenate([first, second], axis=1)


def to_relative(row, z, c):
    first, second = row[:, :512], row[:, 512:]
    mine = jnp.where(c == 0, first, second)
    other = jnp.where(c == 0, second, first)
    return jnp.concatenate([rolled(mine, z, -1), rolled(other, z, -1)], axis=1)


def prepare_kernel(q_in, p_in, positive_in, q_ref, p_ref, q_wide, p_wide, half_ref, index_ref, sems):
    loads = [
        pltpu.make_async_copy(p_in, p_wide, sems.at[16]),
        pltpu.make_async_copy(q_in, q_wide, sems.at[17]),
        pltpu.make_async_copy(positive_in, index_ref, sems.at[18]),
    ]
    for load in loads:
        load.start()
    loads[0].wait()
    half_ref[...] = p_wide[...].astype(jnp.bfloat16)
    copies = [pltpu.make_async_copy(half_ref, p_ref.at[i], sems.at[i]) for i in range(16)]
    for copy in copies:
        copy.start()
    loads[1].wait()
    q_ref[:ROWS, :] = q_wide[...].astype(jnp.bfloat16)
    loads[2].wait()
    index = index_ref[...]
    index = jnp.concatenate([index] * 16, axis=1)
    row = lax.broadcasted_iota(jnp.int32, (PIECE - ROWS, BLOCK), 0)
    meta = jnp.where(row == 0, index >> 7, jnp.where(row == 1, index & 127, 0))
    q_ref[ROWS:, :] = meta.astype(jnp.float32).astype(jnp.bfloat16)
    for copy in copies:
        copy.wait()


def join_kernel(*refs):
    out_ref, at = refs[-1], 0
    for ref in refs[:-1]:
        rows = ref.shape[0]
        out_ref[at : at + rows, :] = ref[...]
        at += rows


def tile(k):
    return slice(k * TILE, (k + 1) * TILE)


def take_queries(ref, q_ref, target_ref, half):
    lane_block = lax.broadcasted_iota(jnp.int32, (1, BLOCK // 2), 1) // ROWS
    high = jnp.zeros((1, BLOCK // 2), jnp.float32)
    low = jnp.zeros((1, BLOCK // 2), jnp.float32)
    for slot in range(8):
        at, to = slot * PIECE, half * (BLOCK // 2) + slot * ROWS
        q_ref[to : to + ROWS, :] = ref[at : at + ROWS, :]
        meta = ref[at + ROWS : at + PIECE, : BLOCK // 2].astype(jnp.float32)
        high = jnp.where(lane_block == slot, meta[0:1], high)
        low = jnp.where(lane_block == slot, meta[1:2], low)
    target = high.astype(jnp.int32) * 128 + low.astype(jnp.int32)
    here = (
        (((target >> 6) & 3) == high_z())
        & (((target >> 8) & 1) == lax.axis_index("c"))
        & (((target >> 11) & 1) == lax.axis_index("zl"))
    )
    column = ((target >> 12) & 3) * 256 + ((target >> 9) & 3) * 64 + (target & 63)
    target_ref[:, half * (BLOCK // 2) : (half + 1) * (BLOCK // 2)] = jnp.where(here, column, -1)


def scores_kernel(
    own_ref, other_in, p_ref, q_ref, target_ref, e_ref, highest_ref, stats_ref, other_ref, sem
):
    load = pltpu.make_async_copy(other_in, other_ref, sem)
    load.start()
    z, c = place()
    take_queries(own_ref, q_ref, target_ref, 0)
    lse, positive = [], []
    for i in range(4):
        if i == 2:
            load.wait()
            take_queries(other_ref, q_ref, target_ref, 1)
        column = target_ref[:, tile(i)]
        highest = jnp.full((1, TILE), -jnp.inf, jnp.float32)
        pos = jnp.zeros((1, TILE), jnp.float32)
        for j in range(4):
            s = logit_scale * lax.dot_general(
                p_ref[tile(j), :], q_ref[tile(i), :], (((1,), (1,)), ((), ())),
                preferred_element_type=jnp.float32,
            )
            e_ref[tile(j), tile(i)] = s
            row = lax.broadcasted_iota(jnp.int32, (TILE, TILE), 0) + j * TILE
            pos = pos + jnp.sum(jnp.where(row == column, s, 0.0), axis=0, keepdims=True)
            highest = jnp.maximum(highest, jnp.max(s, axis=0, keepdims=True))
        acc = jnp.zeros((1, TILE), jnp.float32)
        for j in range(4):
            e = jnp.exp(e_ref[tile(j), tile(i)] - highest)
            e_ref[tile(j), tile(i)] = e
            acc = acc + jnp.sum(e, axis=0, keepdims=True)
        highest_ref[:, tile(i)] = highest
        lse.append(highest + jnp.log(acc))
        positive.append(pos)
    for at, parts in ((0, lse), (8, positive)):
        row = to_absolute(jnp.concatenate(parts, axis=1), z, c)
        for r in range(8):
            stats_ref[0, at + r : at + r + 1, :] = row[:, r * 128 : (r + 1) * 128]
    for k in range(1, 16):
        stats_ref[k] = stats_ref[0]


def weights_kernel(
    stats_ref, target_ref, e_ref, highest_ref, q_ref, p_ref, out_ref, mine_ref, other_ref, loss_ref,
    w_ref, terms_ref, sums_ref, sems,
):
    z, c = place()
    stats = stats_ref[...]
    lses = stats[:, 0:8, :]
    highest = jnp.max(lses, axis=0)
    log_norm = highest + jnp.log(jnp.sum(jnp.exp(lses - highest[None]), axis=0))
    positive = jnp.sum(stats[:, 8:16, :], axis=0)
    log_norm, positive = (
        to_relative(jnp.concatenate([v[r : r + 1] for r in range(8)], axis=1), z, c)
        for v in (log_norm, positive)
    )
    loss_ref[...] = (log_norm - positive)[:, 0:ROWS]
    factor = logit_scale * jnp.exp(highest_ref[...] - log_norm)
    stores = []
    for j in range(4):
        for i in range(4):
            row = lax.broadcasted_iota(jnp.int32, (TILE, TILE), 0) + j * TILE
            taken = jnp.where(row == target_ref[:, tile(i)], logit_scale, 0.0)
            w = e_ref[tile(j), tile(i)] * factor[:, tile(i)] - taken
            w_ref[tile(j), tile(i)] = w.astype(jnp.bfloat16)
        for k in range(4):
            terms_ref[tile(j), tile(k)] = jnp.dot(
                w_ref[tile(j), :], q_ref[:, tile(k)], preferred_element_type=jnp.float32
            ).astype(jnp.bfloat16)
        stores.append(pltpu.make_async_copy(terms_ref.at[tile(j)], out_ref.at[tile(j)], sems.at[j]))
        stores[-1].start()
    for step, i in enumerate((2, 3, 0, 1)):
        for k in range(4):
            sums_ref[tile(i), tile(k)] = lax.dot_general(
                w_ref[:, tile(i)], p_ref[:, tile(k)], (((0,), (0,)), ((), ())),
                preferred_element_type=jnp.float32,
            )
        to_ref = mine_ref if i < 2 else other_ref
        stores.append(
            pltpu.make_async_copy(sums_ref.at[tile(i)], to_ref.at[tile(i % 2)], sems.at[4 + step])
        )
        stores[-1].start()
    for store in stores:
        store.wait()


def split_kernel(slots, mine_in, arrived_in, *rest):
    outs, (mine_ref, arrived_ref, sems) = rest[: len(slots)], rest[len(slots) :]
    loads = []
    for i, slot in enumerate(slots):
        at = slice(slot * ROWS, (slot + 1) * ROWS)
        loads.append(pltpu.make_async_copy(mine_in.at[at], mine_ref.at[i], sems.at[0, i]))
        loads.append(pltpu.make_async_copy(arrived_in.at[at], arrived_ref.at[i], sems.at[1, i]))
    for load in loads:
        load.start()
    for i in range(len(slots)):
        loads[2 * i].wait()
        loads[2 * i + 1].wait()
        outs[i][...] = (mine_ref[i] + arrived_ref[i]).astype(outs[i].dtype)


def total_kernel(p_ref, own_ref, *rest):
    pieces, (q_out, p_out), (sum_ref, sems) = rest[:7], rest[7:9], rest[9:]
    stores = []
    for k in range(4):
        r = slice(k * 16, (k + 1) * 16)
        total = p_ref[0, r, :].astype(jnp.float32)
        for i in range(1, 16):
            total = total + p_ref[i, r, :].astype(jnp.float32)
        sum_ref[1, r, :] = total
        stores.append(pltpu.make_async_copy(sum_ref.at[1, r], p_out.at[r], sems.at[k]))
        stores[-1].start()
    total = own_ref[...]
    for piece in pieces:
        total = total + piece[...].astype(jnp.float32)
    sum_ref[0] = total
    stores.append(pltpu.make_async_copy(sum_ref.at[0], q_out, sems.at[4]))
    stores[-1].start()
    for store in stores:
        store.wait()


def cost(flops, count):
    return pl.CostEstimate(flops=flops, bytes_accessed=count, transcendentals=0)


def struct(shape, dtype):
    return jax.ShapeDtypeStruct(shape, dtype)


def far(shape, dtype):
    return pltpu.HBM(shape, dtype)


def call(kernel, name, args, out_shape, out_specs, limit, flops=1 << 28, scratch=(), held=()):
    return pl.pallas_call(
        kernel,
        out_shape=out_shape,
        in_specs=[HBM if i in held else VMEM for i in range(len(args))],
        out_specs=out_specs,
        scratch_shapes=scratch,
        compiler_params=pltpu.CompilerParams(vmem_limit_bytes=limit << 20),
        cost_estimate=cost(flops, 4 << 20),
        name=name,
    )(*(pltpu.with_memory_space_constraint(a, pltpu.HBM) if i in held else a for i, a in enumerate(args)))


def body(queries, passages, positives):
    width = queries.shape[1]
    matmul = 2 * BLOCK**3
    own, p_sent = call(
        prepare_kernel,
        "prepare",
        (queries, passages, positives.reshape(1, ROWS)),
        (struct((PIECE, width), jnp.bfloat16), far((16, ROWS, width), jnp.bfloat16)),
        (VMEM, HBM),
        limit=4,
        scratch=(
            pltpu.VMEM((ROWS, width), jnp.float32),
            pltpu.VMEM((ROWS, width), jnp.float32),
            pltpu.VMEM((ROWS, width), jnp.bfloat16),
            pltpu.VMEM((1, ROWS), jnp.int32),
            pltpu.SemaphoreType.DMA((19,)),
        ),
        held=(0, 1, 2),
    )
    p_block = lax.all_to_all(p_sent, XY, 0, 0, tiled=True).reshape(BLOCK, width)
    gathered = gather_along_z(own)
    partner = to_partner(gathered)
    q_block, column, scores, highest, stats = call(
        scores_kernel,
        "scores",
        (gathered, partner, p_block),
        (
            struct((BLOCK, width), jnp.bfloat16),
            struct((1, BLOCK), jnp.int32),
            struct((BLOCK, BLOCK), jnp.float32),
            struct((1, BLOCK), jnp.float32),
            struct((16, 16, 128), jnp.float32),
        ),
        (VMEM,) * 5,
        limit=20,
        flops=matmul,
        scratch=(pltpu.VMEM((8 * PIECE, width), jnp.bfloat16), pltpu.SemaphoreType.DMA),
        held=(1,),
    )
    stats = lax.all_to_all(stats, ZC, 0, 0, tiled=True)
    half = (BLOCK // 2, width)
    p_terms, mine, others, losses = call(
        weights_kernel,
        "weights",
        (stats, column, scores, highest, q_block, p_block),
        (
            far((BLOCK, width), jnp.bfloat16),
            far(half, jnp.float32),
            far(half, jnp.float32),
            struct((1, ROWS), jnp.float32),
        ),
        (HBM, HBM, HBM, VMEM),
        limit=30,
        flops=2 * matmul,
        scratch=(
            pltpu.VMEM((BLOCK, BLOCK), jnp.bfloat16),
            pltpu.VMEM((BLOCK, width), jnp.bfloat16),
            pltpu.VMEM((BLOCK, width), jnp.float32),
            pltpu.SemaphoreType.DMA((8,)),
        ),
    )
    p_terms = lax.all_to_all(p_terms.reshape(16, ROWS, width), XY, 0, 0, tiled=True)
    block = (ROWS, width)
    gathered_terms = to_partner(others)

    def split(slots, name):
        wide = (len(slots), *block)
        return call(
            functools.partial(split_kernel, slots),
            name,
            (mine, gathered_terms),
            tuple(struct(block, jnp.bfloat16 if slot else jnp.float32) for slot in slots),
            (VMEM,) * len(slots),
            limit=8,
            scratch=(
                pltpu.VMEM(wide, jnp.float32),
                pltpu.VMEM(wide, jnp.float32),
                pltpu.SemaphoreType.DMA((2, len(slots))),
            ),
            held=(0, 1),
        )

    far_slots, near_slots = (4, 5, 3), (6, 2, 7, 1, 0)
    arrived = [along_z(piece, slot) for slot, piece in zip(far_slots, split(far_slots, "far"))]
    *pieces, own_terms = split(near_slots, "near")
    arrived += [along_z(piece, slot) for slot, piece in zip(near_slots, pieces)]
    query_grads, passage_grads = call(
        total_kernel,
        "total",
        (p_terms, own_terms, *arrived),
        (far(block, jnp.float32),) * 2,
        (HBM,) * 2,
        limit=8,
        scratch=(
            pltpu.VMEM((2, *block), jnp.float32),
            pltpu.SemaphoreType.DMA((5,)),
        ),
    )
    return losses.reshape(ROWS), query_grads, passage_grads


def solution(mesh):
    torus = Mesh(mesh.devices.reshape(4, 2, 4, 2, 2, 2), AXES)
    placed = (P(AXES, None), P(AXES, None), P(AXES))
    return jax.shard_map(
        body,
        mesh=torus,
        in_specs=placed,
        out_specs=(P(AXES), P(AXES, None), P(AXES, None)),
        check_vma=False,
    )
```

```python
import functools

import jax
import jax.numpy as jnp
import numpy as np
from jax import lax
from jax.experimental import pallas as pl
from jax.experimental.pallas import tpu as pltpu
from jax.sharding import Mesh
from jax.sharding import PartitionSpec as P

AXES = ("xa", "xb", "zl", "ya", "yb", "c", "za", "zb")
XY = ("yb", "ya", "xb", "xa")
TARGET_BIT = {"xa": 13, "xb": 12, "ya": 10, "yb": 9}
ZC = ("c", "za", "zb", "zl")

logit_scale = 20.0
ROWS = 64
BLOCK = 1024
TILE = 256
PIECE = 72
VMEM = pl.BlockSpec(memory_space=pltpu.VMEM)
HBM = pl.BlockSpec(memory_space=pltpu.HBM)


def along_z(value, shift):
    pairs = []
    for i in range(8):
        zl, zh = divmod(i, 4)
        to = (zh * 2 + zl + shift) % 8
        pairs.append((i, (to % 2) * 4 + to // 2))
    return lax.ppermute(value, ("zl", "za", "zb"), pairs)


def to_partner(value):
    return lax.ppermute(value, "c", [(0, 1), (1, 0)])


def gather_along_z(own):
    half = 40
    up2, down2 = along_z(own, 2), along_z(own, -2)
    up1, down1 = along_z(own, 1), along_z(own, -1)
    up3, down3 = along_z(up2, 1), along_z(down2, -1)
    far_a, far_b = along_z(up2[:half], 2), along_z(down2[half:], -2)
    pieces = (own, down1, down2, down3, far_a, far_b, up3, up2, up1)
    return call(
        join_kernel, "join", pieces, struct((8 * PIECE, own.shape[1]), jnp.bfloat16), VMEM, limit=8
    )


def rolled(row, z, sign):
    for bit in (1, 2, 4):
        turned = pltpu.roll(row, (sign * bit * ROWS) % 512, 1)
        row = jnp.where((z & bit) != 0, turned, row)
    return row


def high_z():
    return lax.axis_index("za") * 2 + lax.axis_index("zb")


def place():
    z = high_z() * 2 + lax.axis_index("zl")
    return z, lax.axis_index("c")


def to_absolute(row, z, c):
    mine, other = rolled(row[:, :512], z, 1), rolled(row[:, 512:], z, 1)
    first = jnp.where(c == 0, mine, other)
    second = jnp.where(c == 0, other, mine)
    return jnp.concatenate([first, second], axis=1)


def to_relative(row, z, c):
    first, second = row[:, :512], row[:, 512:]
    mine = jnp.where(c == 0, first, second)
    other = jnp.where(c == 0, second, first)
    return jnp.concatenate([rolled(mine, z, -1), rolled(other, z, -1)], axis=1)


def prepare_kernel(q_in, p_in, positive_in, q_ref, p_ref, q_wide, p_wide, half_ref, index_ref, sems):
    loads = [
        pltpu.make_async_copy(p_in, p_wide, sems.at[16]),
        pltpu.make_async_copy(q_in, q_wide, sems.at[17]),
        pltpu.make_async_copy(positive_in, index_ref, sems.at[18]),
    ]
    for load in loads:
        load.start()
    loads[0].wait()
    half_ref[...] = p_wide[...].astype(jnp.bfloat16)
    copies = [pltpu.make_async_copy(half_ref, p_ref.at[i], sems.at[i]) for i in range(16)]
    for copy in copies:
        copy.start()
    loads[1].wait()
    q_ref[:ROWS, :] = q_wide[...].astype(jnp.bfloat16)
    loads[2].wait()
    index = index_ref[...]
    index = jnp.concatenate([index] * 16, axis=1)
    row = lax.broadcasted_iota(jnp.int32, (PIECE - ROWS, BLOCK), 0)
    meta = jnp.where(row == 0, index >> 7, jnp.where(row == 1, index & 127, 0))
    q_ref[ROWS:, :] = meta.astype(jnp.float32).astype(jnp.bfloat16)
    for copy in copies:
        copy.wait()


def join_kernel(*refs):
    out_ref, at = refs[-1], 0
    for ref in refs[:-1]:
        rows = ref.shape[0]
        out_ref[at : at + rows, :] = ref[...]
        at += rows


def tile(k):
    return slice(k * TILE, (k + 1) * TILE)


def take_queries(ref, q_ref, target_ref, half):
    lane_block = lax.broadcasted_iota(jnp.int32, (1, BLOCK // 2), 1) // ROWS
    high = jnp.zeros((1, BLOCK // 2), jnp.float32)
    low = jnp.zeros((1, BLOCK // 2), jnp.float32)
    for slot in range(8):
        at, to = slot * PIECE, half * (BLOCK // 2) + slot * ROWS
        q_ref[to : to + ROWS, :] = ref[at : at + ROWS, :]
        meta = ref[at + ROWS : at + PIECE, : BLOCK // 2].astype(jnp.float32)
        high = jnp.where(lane_block == slot, meta[0:1], high)
        low = jnp.where(lane_block == slot, meta[1:2], low)
    target = high.astype(jnp.int32) * 128 + low.astype(jnp.int32)
    here = (
        (((target >> 6) & 3) == high_z())
        & (((target >> 8) & 1) == lax.axis_index("c"))
        & (((target >> 11) & 1) == lax.axis_index("zl"))
    )
    column = target & (ROWS - 1)
    for place_of, axis in enumerate(XY):
        column = column + (((target >> TARGET_BIT[axis]) & 1) << (9 - place_of))
    target_ref[:, half * (BLOCK // 2) : (half + 1) * (BLOCK // 2)] = jnp.where(here, column, -1)


def scores_kernel(
    own_ref, other_in, p_ref, q_ref, target_ref, e_ref, highest_ref, stats_ref, other_ref, sem
):
    load = pltpu.make_async_copy(other_in, other_ref, sem)
    load.start()
    z, c = place()
    take_queries(own_ref, q_ref, target_ref, 0)
    lse, positive, columns = [], [], []

    def exponentials(i, j):
        e = jnp.exp(e_ref[tile(j), tile(i)] - columns[i][0])
        e_ref[tile(j), tile(i)] = e
        columns[i][1] = columns[i][1] + jnp.sum(e, axis=0, keepdims=True)

    for i in range(5):
        if i == 2:
            load.wait()
            take_queries(other_ref, q_ref, target_ref, 1)
        highest = jnp.full((1, TILE), -jnp.inf, jnp.float32)
        pos = jnp.zeros((1, TILE), jnp.float32)
        for j in range(4):
            if i < 4:
                s = logit_scale * lax.dot_general(
                    p_ref[tile(j), :], q_ref[tile(i), :], (((1,), (1,)), ((), ())),
                    preferred_element_type=jnp.float32,
                )
                e_ref[tile(j), tile(i)] = s
                row = lax.broadcasted_iota(jnp.int32, (TILE, TILE), 0) + j * TILE
                taken = jnp.where(row == target_ref[:, tile(i)], s, 0.0)
                pos = pos + jnp.sum(taken, axis=0, keepdims=True)
                highest = jnp.maximum(highest, jnp.max(s, axis=0, keepdims=True))
            if i > 0:
                exponentials(i - 1, j)
        if i > 0:
            lse.append(columns[i - 1][0] + jnp.log(columns[i - 1][1]))
        if i < 4:
            highest_ref[:, tile(i)] = highest
            positive.append(pos)
            columns.append([highest, jnp.zeros((1, TILE), jnp.float32)])
    for at, parts in ((0, lse), (8, positive)):
        row = to_absolute(jnp.concatenate(parts, axis=1), z, c)
        for r in range(8):
            stats_ref[0, at + r : at + r + 1, :] = row[:, r * 128 : (r + 1) * 128]
    for k in range(1, 16):
        stats_ref[k] = stats_ref[0]


def weights_kernel(
    stats_ref, target_ref, e_ref, highest_ref, q_ref, p_ref, out_ref, mine_ref, other_ref, loss_ref,
    w_ref, terms_ref, sums_ref, sems,
):
    z, c = place()
    stats = stats_ref[...]
    lses = stats[:, 0:8, :]
    highest = jnp.max(lses, axis=0)
    log_norm = highest + jnp.log(jnp.sum(jnp.exp(lses - highest[None]), axis=0))
    positive = jnp.sum(stats[:, 8:16, :], axis=0)
    log_norm, positive = (
        to_relative(jnp.concatenate([v[r : r + 1] for r in range(8)], axis=1), z, c)
        for v in (log_norm, positive)
    )
    loss_ref[...] = (log_norm - positive)[:, 0:ROWS]
    factor = logit_scale * jnp.exp(highest_ref[...] - log_norm)
    stores = []

    def weigh(j, i):
        row = lax.broadcasted_iota(jnp.int32, (TILE, TILE), 0) + j * TILE
        taken = jnp.where(row == target_ref[:, tile(i)], logit_scale, 0.0)
        w = e_ref[tile(j), tile(i)] * factor[:, tile(i)] - taken
        w_ref[tile(j), tile(i)] = w.astype(jnp.bfloat16)

    for i in range(4):
        weigh(0, i)
    for j in range(4):
        for k in range(4):
            if j < 3:
                weigh(j + 1, k)
            terms_ref[tile(j), tile(k)] = jnp.dot(
                w_ref[tile(j), :], q_ref[:, tile(k)], preferred_element_type=jnp.float32
            ).astype(jnp.bfloat16)
        stores.append(pltpu.make_async_copy(terms_ref.at[tile(j)], out_ref.at[tile(j)], sems.at[j]))
        stores[-1].start()
    for step, i in enumerate((2, 3, 0, 1)):
        for k in range(4):
            sums_ref[tile(i), tile(k)] = lax.dot_general(
                w_ref[:, tile(i)], p_ref[:, tile(k)], (((0,), (0,)), ((), ())),
                preferred_element_type=jnp.float32,
            )
        to_ref = mine_ref if i < 2 else other_ref
        stores.append(
            pltpu.make_async_copy(sums_ref.at[tile(i)], to_ref.at[tile(i % 2)], sems.at[4 + step])
        )
        stores[-1].start()
    for store in stores:
        store.wait()


def split_kernel(slots, mine_in, arrived_in, *rest):
    outs, (mine_ref, arrived_ref, sems) = rest[: len(slots)], rest[len(slots) :]
    loads = []
    for i, slot in enumerate(slots):
        at = slice(slot * ROWS, (slot + 1) * ROWS)
        loads.append(pltpu.make_async_copy(mine_in.at[at], mine_ref.at[i], sems.at[0, i]))
        loads.append(pltpu.make_async_copy(arrived_in.at[at], arrived_ref.at[i], sems.at[1, i]))
    for load in loads:
        load.start()
    for i in range(len(slots)):
        loads[2 * i].wait()
        loads[2 * i + 1].wait()
        outs[i][...] = (mine_ref[i] + arrived_ref[i]).astype(outs[i].dtype)


def total_kernel(p_ref, own_ref, *rest):
    pieces, (q_out, p_out), (sum_ref, sems) = rest[:7], rest[7:9], rest[9:]
    stores = []
    for k in range(4):
        r = slice(k * 16, (k + 1) * 16)
        total = p_ref[0, r, :].astype(jnp.float32)
        for i in range(1, 16):
            total = total + p_ref[i, r, :].astype(jnp.float32)
        sum_ref[1, r, :] = total
        stores.append(pltpu.make_async_copy(sum_ref.at[1, r], p_out.at[r], sems.at[k]))
        stores[-1].start()
    total = own_ref[...]
    for piece in pieces:
        total = total + piece[...].astype(jnp.float32)
    sum_ref[0] = total
    stores.append(pltpu.make_async_copy(sum_ref.at[0], q_out, sems.at[4]))
    stores[-1].start()
    for store in stores:
        store.wait()


def cost(flops, count):
    return pl.CostEstimate(flops=flops, bytes_accessed=count, transcendentals=0)


def struct(shape, dtype):
    return jax.ShapeDtypeStruct(shape, dtype)


def far(shape, dtype):
    return pltpu.HBM(shape, dtype)


def call(kernel, name, args, out_shape, out_specs, limit, flops=1 << 28, scratch=(), held=()):
    return pl.pallas_call(
        kernel,
        out_shape=out_shape,
        in_specs=[HBM if i in held else VMEM for i in range(len(args))],
        out_specs=out_specs,
        scratch_shapes=scratch,
        compiler_params=pltpu.CompilerParams(vmem_limit_bytes=limit << 20),
        cost_estimate=cost(flops, 4 << 20),
        name=name,
    )(*(pltpu.with_memory_space_constraint(a, pltpu.HBM) if i in held else a for i, a in enumerate(args)))


def body(queries, passages, positives):
    width = queries.shape[1]
    matmul = 2 * BLOCK**3
    own, p_sent = call(
        prepare_kernel,
        "prepare",
        (queries, passages, positives.reshape(1, ROWS)),
        (struct((PIECE, width), jnp.bfloat16), far((16, ROWS, width), jnp.bfloat16)),
        (VMEM, HBM),
        limit=4,
        scratch=(
            pltpu.VMEM((ROWS, width), jnp.float32),
            pltpu.VMEM((ROWS, width), jnp.float32),
            pltpu.VMEM((ROWS, width), jnp.bfloat16),
            pltpu.VMEM((1, ROWS), jnp.int32),
            pltpu.SemaphoreType.DMA((19,)),
        ),
        held=(0, 1, 2),
    )
    p_block = lax.all_to_all(p_sent, XY, 0, 0, tiled=True).reshape(BLOCK, width)
    gathered = gather_along_z(own)
    partner = to_partner(gathered)
    q_block, column, scores, highest, stats = call(
        scores_kernel,
        "scores",
        (gathered, partner, p_block),
        (
            struct((BLOCK, width), jnp.bfloat16),
            struct((1, BLOCK), jnp.int32),
            struct((BLOCK, BLOCK), jnp.float32),
            struct((1, BLOCK), jnp.float32),
            struct((16, 16, 128), jnp.float32),
        ),
        (VMEM,) * 5,
        limit=20,
        flops=matmul,
        scratch=(pltpu.VMEM((8 * PIECE, width), jnp.bfloat16), pltpu.SemaphoreType.DMA),
        held=(1,),
    )
    stats = lax.all_to_all(stats, ZC, 0, 0, tiled=True)
    half = (BLOCK // 2, width)
    p_terms, mine, others, losses = call(
        weights_kernel,
        "weights",
        (stats, column, scores, highest, q_block, p_block),
        (
            far((BLOCK, width), jnp.bfloat16),
            far(half, jnp.float32),
            far(half, jnp.float32),
            struct((1, ROWS), jnp.float32),
        ),
        (HBM, HBM, HBM, VMEM),
        limit=30,
        flops=2 * matmul,
        scratch=(
            pltpu.VMEM((BLOCK, BLOCK), jnp.bfloat16),
            pltpu.VMEM((BLOCK, width), jnp.bfloat16),
            pltpu.VMEM((BLOCK, width), jnp.float32),
            pltpu.SemaphoreType.DMA((8,)),
        ),
    )
    p_terms = lax.all_to_all(p_terms.reshape(16, ROWS, width), XY, 0, 0, tiled=True)
    block = (ROWS, width)
    gathered_terms = to_partner(others)

    def split(slots, name):
        wide = (len(slots), *block)
        return call(
            functools.partial(split_kernel, slots),
            name,
            (mine, gathered_terms),
            tuple(struct(block, jnp.bfloat16 if slot else jnp.float32) for slot in slots),
            (VMEM,) * len(slots),
            limit=8,
            scratch=(
                pltpu.VMEM(wide, jnp.float32),
                pltpu.VMEM(wide, jnp.float32),
                pltpu.SemaphoreType.DMA((2, len(slots))),
            ),
            held=(0, 1),
        )

    far_slots, near_slots = (4, 5, 3), (6, 2, 7, 1, 0)
    arrived = [along_z(piece, slot) for slot, piece in zip(far_slots, split(far_slots, "far"))]
    *pieces, own_terms = split(near_slots, "near")
    arrived += [along_z(piece, slot) for slot, piece in zip(near_slots, pieces)]
    query_grads, passage_grads = call(
        total_kernel,
        "total",
        (p_terms, own_terms, *arrived),
        (far(block, jnp.float32),) * 2,
        (HBM,) * 2,
        limit=8,
        scratch=(
            pltpu.VMEM((2, *block), jnp.float32),
            pltpu.SemaphoreType.DMA((5,)),
        ),
    )
    return losses.reshape(ROWS), query_grads, passage_grads


def solution(mesh):
    torus = Mesh(mesh.devices.reshape((2,) * 8), AXES)
    placed = (P(AXES, None), P(AXES, None), P(AXES))
    return jax.shard_map(
        body,
        mesh=torus,
        in_specs=placed,
        out_specs=(P(AXES), P(AXES, None), P(AXES, None)),
        check_vma=False,
    )
```

```python
import functools

import jax
import jax.numpy as jnp
import numpy as np
from jax import lax
from jax.experimental import pallas as pl
from jax.experimental.pallas import tpu as pltpu
from jax.sharding import Mesh
from jax.sharding import PartitionSpec as P

AXES = ("xa", "xb", "zl", "ya", "yb", "c", "za", "zb")
XY = ("yb", "ya", "xb", "xa")
TARGET_BIT = {"xa": 13, "xb": 12, "ya": 10, "yb": 9}
ZC = ("zb", "zl", "c", "za")

logit_scale = 20.0
ROWS = 64
BLOCK = 1024
TILE = 256
PIECE = 72
VMEM = pl.BlockSpec(memory_space=pltpu.VMEM)
HBM = pl.BlockSpec(memory_space=pltpu.HBM)


def along_z(value, shift):
    pairs = []
    for i in range(8):
        zl, zh = divmod(i, 4)
        to = (zh * 2 + zl + shift) % 8
        pairs.append((i, (to % 2) * 4 + to // 2))
    return lax.ppermute(value, ("zl", "za", "zb"), pairs)


def to_partner(value):
    return lax.ppermute(value, "c", [(0, 1), (1, 0)])


def gather_along_z(own):
    half = 40
    up2, down2 = along_z(own, 2), along_z(own, -2)
    up1, down1 = along_z(own, 1), along_z(own, -1)
    up3, down3 = along_z(up2, 1), along_z(down2, -1)
    far_a, far_b = along_z(up2[:half], 2), along_z(down2[half:], -2)
    pieces = (own, down1, down2, down3, far_a, far_b, up3, up2, up1)
    return call(
        join_kernel, "join", pieces, struct((8 * PIECE, own.shape[1]), jnp.bfloat16), VMEM, limit=8
    )


def rolled(row, z, sign):
    for bit in (1, 2, 4):
        turned = pltpu.roll(row, (sign * bit * ROWS) % 512, 1)
        row = jnp.where((z & bit) != 0, turned, row)
    return row


def high_z():
    return lax.axis_index("za") * 2 + lax.axis_index("zb")


def place():
    z = high_z() * 2 + lax.axis_index("zl")
    return z, lax.axis_index("c")


def to_absolute(row, z, c):
    mine, other = rolled(row[:, :512], z, 1), rolled(row[:, 512:], z, 1)
    first = jnp.where(c == 0, mine, other)
    second = jnp.where(c == 0, other, mine)
    return jnp.concatenate([first, second], axis=1)


def to_relative(row, z, c):
    first, second = row[:, :512], row[:, 512:]
    mine = jnp.where(c == 0, first, second)
    other = jnp.where(c == 0, second, first)
    return jnp.concatenate([rolled(mine, z, -1), rolled(other, z, -1)], axis=1)


def prepare_kernel(q_in, p_in, positive_in, q_ref, p_ref, q_wide, p_wide, half_ref, index_ref, sems):
    loads = [
        pltpu.make_async_copy(p_in, p_wide, sems.at[16]),
        pltpu.make_async_copy(q_in, q_wide, sems.at[17]),
        pltpu.make_async_copy(positive_in, index_ref, sems.at[18]),
    ]
    for load in loads:
        load.start()
    loads[0].wait()
    half_ref[...] = p_wide[...].astype(jnp.bfloat16)
    copies = [pltpu.make_async_copy(half_ref, p_ref.at[i], sems.at[i]) for i in range(16)]
    for copy in copies:
        copy.start()
    loads[1].wait()
    q_ref[:ROWS, :] = q_wide[...].astype(jnp.bfloat16)
    loads[2].wait()
    index = index_ref[...]
    index = jnp.concatenate([index] * 16, axis=1)
    row = lax.broadcasted_iota(jnp.int32, (PIECE - ROWS, BLOCK), 0)
    meta = jnp.where(row == 0, index >> 7, jnp.where(row == 1, index & 127, 0))
    q_ref[ROWS:, :] = meta.astype(jnp.float32).astype(jnp.bfloat16)
    for copy in copies:
        copy.wait()


def join_kernel(*refs):
    out_ref, at = refs[-1], 0
    for ref in refs[:-1]:
        rows = ref.shape[0]
        out_ref[at : at + rows, :] = ref[...]
        at += rows


def tile(k):
    return slice(k * TILE, (k + 1) * TILE)


def take_queries(ref, q_ref, target_ref, half):
    lane_block = lax.broadcasted_iota(jnp.int32, (1, BLOCK // 2), 1) // ROWS
    high = jnp.zeros((1, BLOCK // 2), jnp.float32)
    low = jnp.zeros((1, BLOCK // 2), jnp.float32)
    for slot in range(8):
        at, to = slot * PIECE, half * (BLOCK // 2) + slot * ROWS
        q_ref[to : to + ROWS, :] = ref[at : at + ROWS, :]
        meta = ref[at + ROWS : at + PIECE, : BLOCK // 2].astype(jnp.float32)
        high = jnp.where(lane_block == slot, meta[0:1], high)
        low = jnp.where(lane_block == slot, meta[1:2], low)
    target = high.astype(jnp.int32) * 128 + low.astype(jnp.int32)
    here = (
        (((target >> 6) & 3) == high_z())
        & (((target >> 8) & 1) == lax.axis_index("c"))
        & (((target >> 11) & 1) == lax.axis_index("zl"))
    )
    column = target & (ROWS - 1)
    for place_of, axis in enumerate(XY):
        column = column + (((target >> TARGET_BIT[axis]) & 1) << (9 - place_of))
    target_ref[:, half * (BLOCK // 2) : (half + 1) * (BLOCK // 2)] = jnp.where(here, column, -1)


def scores_kernel(
    own_ref, other_in, p_ref, q_ref, target_ref, e_ref, highest_ref, stats_ref, other_ref, sem
):
    load = pltpu.make_async_copy(other_in, other_ref, sem)
    load.start()
    z, c = place()
    take_queries(own_ref, q_ref, target_ref, 0)
    lse, positive, columns = [], [], []

    def exponentials(i, j):
        e = jnp.exp(e_ref[tile(j), tile(i)] - columns[i][0])
        e_ref[tile(j), tile(i)] = e
        columns[i][1] = columns[i][1] + jnp.sum(e, axis=0, keepdims=True)

    for i in range(5):
        if i == 2:
            load.wait()
            take_queries(other_ref, q_ref, target_ref, 1)
        highest = jnp.full((1, TILE), -jnp.inf, jnp.float32)
        pos = jnp.zeros((1, TILE), jnp.float32)
        for j in range(4):
            if i < 4:
                s = logit_scale * lax.dot_general(
                    p_ref[tile(j), :], q_ref[tile(i), :], (((1,), (1,)), ((), ())),
                    preferred_element_type=jnp.float32,
                )
                e_ref[tile(j), tile(i)] = s
                row = lax.broadcasted_iota(jnp.int32, (TILE, TILE), 0) + j * TILE
                taken = jnp.where(row == target_ref[:, tile(i)], s, 0.0)
                pos = pos + jnp.sum(taken, axis=0, keepdims=True)
                highest = jnp.maximum(highest, jnp.max(s, axis=0, keepdims=True))
            if i > 0:
                exponentials(i - 1, j)
        if i > 0:
            lse.append(columns[i - 1][0] + jnp.log(columns[i - 1][1]))
        if i < 4:
            highest_ref[:, tile(i)] = highest
            positive.append(pos)
            columns.append([highest, jnp.zeros((1, TILE), jnp.float32)])
    for at, parts in ((0, lse), (8, positive)):
        row = to_absolute(jnp.concatenate(parts, axis=1), z, c)
        for r in range(8):
            stats_ref[0, at + r : at + r + 1, :] = row[:, r * 128 : (r + 1) * 128]
    for k in range(1, 16):
        stats_ref[k] = stats_ref[0]


def weights_kernel(
    stats_ref, target_ref, e_ref, highest_ref, q_ref, p_ref, out_ref, mine_ref, other_ref, loss_ref,
    w_ref, terms_ref, sums_ref, sems,
):
    z, c = place()
    stats = stats_ref[...]
    lses = stats[:, 0:8, :]
    highest = jnp.max(lses, axis=0)
    log_norm = highest + jnp.log(jnp.sum(jnp.exp(lses - highest[None]), axis=0))
    positive = jnp.sum(stats[:, 8:16, :], axis=0)
    log_norm, positive = (
        to_relative(jnp.concatenate([v[r : r + 1] for r in range(8)], axis=1), z, c)
        for v in (log_norm, positive)
    )
    loss_ref[...] = (log_norm - positive)[:, 0:ROWS]
    factor = logit_scale * jnp.exp(highest_ref[...] - log_norm)
    stores = []

    def weigh(j, i):
        row = lax.broadcasted_iota(jnp.int32, (TILE, TILE), 0) + j * TILE
        taken = jnp.where(row == target_ref[:, tile(i)], logit_scale, 0.0)
        w = e_ref[tile(j), tile(i)] * factor[:, tile(i)] - taken
        w_ref[tile(j), tile(i)] = w.astype(jnp.bfloat16)

    for i in range(4):
        weigh(0, i)
    for j in range(4):
        for k in range(4):
            if j < 3:
                weigh(j + 1, k)
            terms_ref[tile(j), tile(k)] = jnp.dot(
                w_ref[tile(j), :], q_ref[:, tile(k)], preferred_element_type=jnp.float32
            ).astype(jnp.bfloat16)
        stores.append(pltpu.make_async_copy(terms_ref.at[tile(j)], out_ref.at[tile(j)], sems.at[j]))
        stores[-1].start()
    for step, i in enumerate((2, 3, 0, 1)):
        for k in range(4):
            sums_ref[tile(i), tile(k)] = lax.dot_general(
                w_ref[:, tile(i)], p_ref[:, tile(k)], (((0,), (0,)), ((), ())),
                preferred_element_type=jnp.float32,
            )
        to_ref = mine_ref if i < 2 else other_ref
        stores.append(
            pltpu.make_async_copy(sums_ref.at[tile(i)], to_ref.at[tile(i % 2)], sems.at[4 + step])
        )
        stores[-1].start()
    for store in stores:
        store.wait()


def split_kernel(slots, mine_in, arrived_in, *rest):
    outs, (mine_ref, arrived_ref, sems) = rest[: len(slots)], rest[len(slots) :]
    loads = []
    for i, slot in enumerate(slots):
        at = slice(slot * ROWS, (slot + 1) * ROWS)
        loads.append(pltpu.make_async_copy(mine_in.at[at], mine_ref.at[i], sems.at[0, i]))
        loads.append(pltpu.make_async_copy(arrived_in.at[at], arrived_ref.at[i], sems.at[1, i]))
    for load in loads:
        load.start()
    for i in range(len(slots)):
        loads[2 * i].wait()
        loads[2 * i + 1].wait()
        outs[i][...] = (mine_ref[i] + arrived_ref[i]).astype(outs[i].dtype)


def total_kernel(p_ref, own_ref, *rest):
    pieces, (q_out, p_out), (sum_ref, sems) = rest[:7], rest[7:9], rest[9:]
    stores = []
    for k in range(4):
        r = slice(k * 16, (k + 1) * 16)
        total = p_ref[0, r, :].astype(jnp.float32)
        for i in range(1, 16):
            total = total + p_ref[i, r, :].astype(jnp.float32)
        sum_ref[1, r, :] = total
        stores.append(pltpu.make_async_copy(sum_ref.at[1, r], p_out.at[r], sems.at[k]))
        stores[-1].start()
    total = own_ref[...]
    for piece in pieces:
        total = total + piece[...].astype(jnp.float32)
    sum_ref[0] = total
    stores.append(pltpu.make_async_copy(sum_ref.at[0], q_out, sems.at[4]))
    stores[-1].start()
    for store in stores:
        store.wait()


def cost(flops, count):
    return pl.CostEstimate(flops=flops, bytes_accessed=count, transcendentals=0)


def struct(shape, dtype):
    return jax.ShapeDtypeStruct(shape, dtype)


def far(shape, dtype):
    return pltpu.HBM(shape, dtype)


def call(kernel, name, args, out_shape, out_specs, limit, flops=1 << 28, scratch=(), held=()):
    return pl.pallas_call(
        kernel,
        out_shape=out_shape,
        in_specs=[HBM if i in held else VMEM for i in range(len(args))],
        out_specs=out_specs,
        scratch_shapes=scratch,
        compiler_params=pltpu.CompilerParams(vmem_limit_bytes=limit << 20),
        cost_estimate=cost(flops, 4 << 20),
        name=name,
    )(*(pltpu.with_memory_space_constraint(a, pltpu.HBM) if i in held else a for i, a in enumerate(args)))


def body(queries, passages, positives):
    width = queries.shape[1]
    matmul = 2 * BLOCK**3
    own, p_sent = call(
        prepare_kernel,
        "prepare",
        (queries, passages, positives.reshape(1, ROWS)),
        (struct((PIECE, width), jnp.bfloat16), far((16, ROWS, width), jnp.bfloat16)),
        (VMEM, HBM),
        limit=4,
        scratch=(
            pltpu.VMEM((ROWS, width), jnp.float32),
            pltpu.VMEM((ROWS, width), jnp.float32),
            pltpu.VMEM((ROWS, width), jnp.bfloat16),
            pltpu.VMEM((1, ROWS), jnp.int32),
            pltpu.SemaphoreType.DMA((19,)),
        ),
        held=(0, 1, 2),
    )
    p_block = lax.all_to_all(p_sent, XY, 0, 0, tiled=True).reshape(BLOCK, width)
    gathered = gather_along_z(own)
    partner = to_partner(gathered)
    q_block, column, scores, highest, stats = call(
        scores_kernel,
        "scores",
        (gathered, partner, p_block),
        (
            struct((BLOCK, width), jnp.bfloat16),
            struct((1, BLOCK), jnp.int32),
            struct((BLOCK, BLOCK), jnp.float32),
            struct((1, BLOCK), jnp.float32),
            struct((16, 16, 128), jnp.float32),
        ),
        (VMEM,) * 5,
        limit=20,
        flops=matmul,
        scratch=(pltpu.VMEM((8 * PIECE, width), jnp.bfloat16), pltpu.SemaphoreType.DMA),
        held=(1,),
    )
    stats = lax.all_to_all(stats, ZC, 0, 0, tiled=True)
    half = (BLOCK // 2, width)
    p_terms, mine, others, losses = call(
        weights_kernel,
        "weights",
        (stats, column, scores, highest, q_block, p_block),
        (
            far((BLOCK, width), jnp.bfloat16),
            far(half, jnp.float32),
            far(half, jnp.float32),
            struct((1, ROWS), jnp.float32),
        ),
        (HBM, HBM, HBM, VMEM),
        limit=30,
        flops=2 * matmul,
        scratch=(
            pltpu.VMEM((BLOCK, BLOCK), jnp.bfloat16),
            pltpu.VMEM((BLOCK, width), jnp.bfloat16),
            pltpu.VMEM((BLOCK, width), jnp.float32),
            pltpu.SemaphoreType.DMA((8,)),
        ),
    )
    p_terms = lax.all_to_all(p_terms.reshape(16, ROWS, width), XY, 0, 0, tiled=True)
    block = (ROWS, width)
    gathered_terms = to_partner(others)

    def split(slots, name):
        wide = (len(slots), *block)
        return call(
            functools.partial(split_kernel, slots),
            name,
            (mine, gathered_terms),
            tuple(struct(block, jnp.bfloat16 if slot else jnp.float32) for slot in slots),
            (VMEM,) * len(slots),
            limit=8,
            scratch=(
                pltpu.VMEM(wide, jnp.float32),
                pltpu.VMEM(wide, jnp.float32),
                pltpu.SemaphoreType.DMA((2, len(slots))),
            ),
            held=(0, 1),
        )

    far_slots, near_slots = (4, 5, 3), (6, 2, 7, 1, 0)
    arrived = [along_z(piece, slot) for slot, piece in zip(far_slots, split(far_slots, "far"))]
    *pieces, own_terms = split(near_slots, "near")
    arrived += [along_z(piece, slot) for slot, piece in zip(near_slots, pieces)]
    query_grads, passage_grads = call(
        total_kernel,
        "total",
        (p_terms, own_terms, *arrived),
        (far(block, jnp.float32),) * 2,
        (HBM,) * 2,
        limit=8,
        scratch=(
            pltpu.VMEM((2, *block), jnp.float32),
            pltpu.SemaphoreType.DMA((5,)),
        ),
    )
    return losses.reshape(ROWS), query_grads, passage_grads


def solution(mesh):
    torus = Mesh(mesh.devices.reshape((2,) * 8), AXES)
    placed = (P(AXES, None), P(AXES, None), P(AXES))
    return jax.shard_map(
        body,
        mesh=torus,
        in_specs=placed,
        out_specs=(P(AXES), P(AXES, None), P(AXES, None)),
        check_vma=False,
    )
```
